512 devices in a mesh: groups: 2 (over y), seq: 16 (over z), heads: 8 (over x), sub: 2 (over core).
Axes of the slice: x: 8, y: 2, z: 16, core: 2. Of those that a mesh axis runs over, the one named last changes fastest.
The devices are a block of a 8x8x16 slice.
Arguments:
- queries: bfloat16 [8192, 8192], P(('groups', 'seq', 'sub'), 'heads'), parts along dimension 0, may hold values from -400 to 400
- keys: bfloat16 [8192, 1024], P(('groups', 'seq', 'sub'), 'heads'), parts along dimension 0, may hold values from -6 to 6
- values: bfloat16 [8192, 1024], P(('groups', 'seq', 'sub'), 'heads'), parts along dimension 0, may hold values from -18 to 18
- half_order: int32 [128], P('groups'), parts along dimension 0, may hold values from 0 to 63, as said below
- frame_lengths: int32 [64], P('groups'), parts along dimension 0, may hold values from 1 to 256, 4096 in all
- out_proj: bfloat16 [8192, 4096], P('heads', ('seq', 'sub')), may hold values from -0.125 to 0.125
- residual_in: bfloat16 [8192, 4096], P(('groups', 'seq', 'sub'), 'heads'), parts along dimension 0, may hold values from -40 to 40
- norm_gain: float32 [4096], P('heads'), may hold values from 0.5 to 1.5
Outputs:
- attended: bfloat16 [8192, 8192], P(('groups', 'seq', 'sub'), 'heads'), parts along dimension 0
- hidden_state: bfloat16 [8192, 4096], P(('groups', 'seq', 'sub'), 'heads'), parts along dimension 0
- normed: bfloat16 [8192, 4096], P(('groups', 'seq', 'sub'), 'heads'), parts along dimension 0
The draws below stay inside these ranges and needn't reach their ends.
There are 2 independent parts, one for each index of `groups`. The reference program is written for one: setup_inputs(seed, part) draws one part's arguments, and reference() takes and returns one part's arrays. A program takes and returns all parts, laid end to end along the dimension named above; an argument that names none is the same for every part. Nothing has to cross between parts.
Inputs may be any that keep to these rules, and one draw needn't show every extreme that they name: `half_order`: a permutation of 0 to 63.
All inputs are finite; a program needn't handle non-finite values.
Results may differ from the reference program's by a relative error of at most 0.005.
Values may be sent and summed in bfloat16 or wider, within the bound.
A program may use at most 64 MiB of HBM per device.

```python
import math
import jax
import jax.numpy as jnp
import numpy as np
from jax import lax

QUERY_HEAD_COUNT = 64
KEY_VALUE_HEADS = 8
HEAD_WIDTH = 128
OUT_WIDTH = 4096
CLIP_TOKENS = 4096
HALF = 64
HALVES = 64
FRAMES = 32
FRAME_MOST = 256


def order_table(key):
    return jax.random.permutation(jax.random.fold_in(key, 11), HALVES).astype(jnp.int32)


def draw_half_order(key, part):
    return order_table(key)


def draw_keys(key, part):
    filled_rows = jax.random.normal(jax.random.fold_in(key, 17), (CLIP_TOKENS, KEY_VALUE_HEADS * HEAD_WIDTH), jnp.float32)
    return jnp.clip(filled_rows, -6.0, 6.0).astype(jnp.bfloat16)


def draw_queries(key, part):
    filled_rows = 1.5 * jax.random.normal(jax.random.fold_in(key, 31), (CLIP_TOKENS, QUERY_HEAD_COUNT * HEAD_WIDTH), jnp.float32)
    return jnp.clip(filled_rows, -400.0, 400.0).astype(jnp.bfloat16)


def draw_residual_in(key, part):
    column_base = jnp.exp(math.log(4.0) * jnp.arange(OUT_WIDTH, dtype=jnp.float32) / OUT_WIDTH) * 0.5
    column_jitter = jnp.exp(jax.random.uniform(jax.random.fold_in(key, 41), (OUT_WIDTH,), jnp.float32, math.log(0.7), math.log(1.4)))
    entries = jax.random.normal(jax.random.fold_in(key, 43), (CLIP_TOKENS, OUT_WIDTH), jnp.float32)
    row_scale = jnp.exp(jax.random.uniform(jax.random.fold_in(key, 47), (CLIP_TOKENS,), jnp.float32, 0.0, math.log(10.0)))
    filled_rows = entries * (column_base * column_jitter)[None, :] * row_scale[:, None]
    return jnp.clip(filled_rows, -40.0, 40.0).astype(jnp.bfloat16)


def strengthened(values, key, source, target, parts, factor):
    owner, partner = [(jnp.arange(values.shape[dim]) // (values.shape[dim] // parts)).reshape([-1 if axis == dim else 1 for axis in range(values.ndim)]) for dim in (source, target)]
    chosen = jax.random.permutation(key, parts)[partner]
    strong = (owner == chosen) | (owner == (partner + parts // 2) % parts)
    return jnp.where(strong, factor * values, values)


def block_scale(stream_key, shape, split, least, top_value):
    loudness, own = 1.0, jax.random.fold_in(stream_key, 6)
    for dim, parts in split:
        draws = jnp.exp(jax.random.uniform(jax.random.fold_in(own, dim), (parts,), jnp.float32, least / len(split), top_value / len(split)))
        loudness = loudness * jnp.repeat(draws, shape[dim] // parts).reshape([-1 if axis == dim else 1 for axis in range(len(shape))])
    return loudness


def profile(count, total, most, skew):
    loads = [(1 << 20) // math.isqrt(grade ** skew) + 1 for grade in range(2, count + 1)]
    spare, counts = total - most - (count - 1), [1] * (count - 1)
    while spare > 0:
        free = [i for i in range(count - 1) if counts[i] < most]
        whole, budget = sum([loads[i] for i in free]), spare
        for i in free:
            more = min(most - counts[i], max(1, budget * loads[i] // whole), spare)
            counts[i] = counts[i] + more
            spare = spare - more
    return np.array([most] + counts)


def ragged(own_key, count, total, reach, slope):
    if count == 2:
        one = jax.random.randint(own_key, (), max(1, total - reach), min(reach, total - 1) + 1)
        return jnp.stack([one, total - one])
    sizes = jnp.asarray(profile(count, total, reach, slope), jnp.int32)
    couples = (count - 1) // 2
    source_of, taker = sizes[1:1 + 2 * couples:2], sizes[2:2 + 2 * couples:2]
    slack = jnp.minimum(source_of - 1, reach - taker)
    passed = jax.random.randint(jax.random.fold_in(own_key, 1), (couples,), 0, 1 << 20) % (slack + 1)
    sizes = sizes.at[1:1 + 2 * couples:2].set(source_of - passed).at[2:2 + 2 * couples:2].set(taker + passed)
    return sizes[jax.random.permutation(jax.random.fold_in(own_key, 2), count)]


def normal_values(key, shape, scale, limit, pieces=(), held_as=jnp.bfloat16):
    gain = block_scale(key, shape, pieces, -0.22, 0.18) if pieces else 1.0
    array = jax.random.normal(key, shape, jnp.float32) * scale * gain
    return jnp.minimum(jnp.maximum(array, -limit), limit).astype(held_as)


def gaussian_with(own_key, extent, deviation, most, cuts, heavy, held_as=jnp.bfloat16):
    array = deviation * jax.random.normal(own_key, extent, jnp.float32)
    if cuts:
        array = array * block_scale(own_key, extent, cuts, -0.22, 0.18)
    return jnp.clip(strengthened(array, jax.random.fold_in(own_key, 3), *heavy), -most, most).astype(held_as)


def setup_inputs(seed: int = 0, part: int = 0) -> dict:
    arg_keys = jax.random.split(jax.random.key(seed), 9)
    part_keys = jax.random.split(jax.random.fold_in(arg_keys[8], part), 9)
    queries = draw_queries(jax.random.fold_in(jax.random.fold_in(arg_keys[8], part), 71), part)
    keys = draw_keys(jax.random.fold_in(jax.random.fold_in(arg_keys[8], part), 71), part)
    values = normal_values(part_keys[2], (CLIP_TOKENS, KEY_VALUE_HEADS * HEAD_WIDTH), 3.0, 18.0, ((0, 32), (1, 8)))
    half_order = draw_half_order(jax.random.fold_in(jax.random.fold_in(arg_keys[8], part), 71), part)
    frame_lengths = ragged(part_keys[4], FRAMES, CLIP_TOKENS, FRAME_MOST, 2).astype(jnp.int32)
    out_proj = gaussian_with(arg_keys[5], (QUERY_HEAD_COUNT * HEAD_WIDTH, OUT_WIDTH), (QUERY_HEAD_COUNT * HEAD_WIDTH) ** -0.5, 0.125, ((0, 8), (1, 32)), (0, 1, 32, 2.75))
    residual_in = draw_residual_in(jax.random.fold_in(jax.random.fold_in(arg_keys[8], part), 71), part)
    norm_gain = jnp.clip(1.0 + 0.1 * jax.random.normal(arg_keys[7], (OUT_WIDTH,), jnp.float32), 0.5, 1.5)
    return dict(queries=queries, keys=keys, values=values, half_order=half_order, frame_lengths=frame_lengths, out_proj=out_proj, residual_in=residual_in, norm_gain=norm_gain)


def positions_of(half_order):
    row_ids = jnp.arange(CLIP_TOKENS, dtype=jnp.int32)
    return (half_order[row_ids // HALF] * HALF + row_ids % HALF).astype(jnp.int32)

def frame_limits(position, frame_lengths):
    frame_ends = jnp.cumsum(frame_lengths).astype(jnp.int32)
    frame_starts = frame_ends - frame_lengths
    chosen = jnp.where(frame_starts[None, :] <= position[:, None], frame_lengths[None, :], 0)
    return lax.optimization_barrier(jnp.sum(chosen, axis=1)).astype(jnp.int32)

def reference(queries, keys, values, half_order, frame_lengths, out_proj, residual_in, norm_gain):
    group_width = QUERY_HEAD_COUNT // KEY_VALUE_HEADS
    position = positions_of(half_order)
    frame_end = frame_limits(position, frame_lengths)
    query_head_rows = queries.reshape(CLIP_TOKENS, KEY_VALUE_HEADS, group_width, HEAD_WIDTH)
    key_head_rows = keys.reshape(CLIP_TOKENS, KEY_VALUE_HEADS, HEAD_WIDTH)
    value_head_rows = values.reshape(CLIP_TOKENS, KEY_VALUE_HEADS, HEAD_WIDTH)
    block_rows = min(512, CLIP_TOKENS)
    block_count = CLIP_TOKENS // block_rows

    def single_head(kv_head):
        key_one = key_head_rows[:, kv_head].astype(jnp.float32)
        value_one = value_head_rows[:, kv_head].astype(jnp.float32)
        query_one = query_head_rows[:, kv_head]

        def one_block(block_id):
            query_block = lax.dynamic_slice_in_dim(query_one, block_id * block_rows, block_rows, 0).astype(jnp.float32)
            limit_block = lax.dynamic_slice_in_dim(frame_end, block_id * block_rows, block_rows, 0)
            scores = jnp.einsum('qgd,kd->gqk', query_block, key_one) * HEAD_WIDTH ** (-0.5)
            visible = position[None, :] < limit_block[:, None]
            scores = jnp.where(visible[None], scores, -1e+30)
            row_max = lax.optimization_barrier(jnp.max(scores, axis=-1, keepdims=True))
            weights = jnp.where(visible[None], jnp.exp(scores - row_max), 0.0)
            total = lax.optimization_barrier(jnp.sum(weights, axis=-1))
            rounded = weights.astype(jnp.bfloat16).astype(jnp.float32)
            summed = jnp.einsum('gqk,kd->qgd', rounded, value_one)
            return (summed / jnp.transpose(total)[:, :, None]).astype(jnp.bfloat16)
        blocks = lax.map(one_block, jnp.arange(block_count, dtype=jnp.int32))
        return blocks.reshape(CLIP_TOKENS, group_width, HEAD_WIDTH)
    each_head_rows = lax.map(single_head, jnp.arange(KEY_VALUE_HEADS, dtype=jnp.int32))
    attended = jnp.transpose(each_head_rows, (1, 0, 2, 3)).reshape(CLIP_TOKENS, QUERY_HEAD_COUNT * HEAD_WIDTH)
    projected = jnp.dot(attended, out_proj, preferred_element_type=jnp.float32)
    hidden_state = (residual_in.astype(jnp.float32) + projected).astype(jnp.bfloat16)
    widened = hidden_state.astype(jnp.float32)
    energy = lax.optimization_barrier(jnp.sum(widened * widened, axis=-1)) / OUT_WIDTH
    normed = (widened * lax.rsqrt(energy + 1e-06)[:, None] * norm_gain.astype(jnp.float32)[None, :]).astype(jnp.bfloat16)
    return (attended, hidden_state, normed)
```

```python
import functools

import jax
import jax.numpy as jnp
from jax import lax
from jax.experimental import pallas as pl
from jax.experimental.pallas import tpu as pltpu
from jax.sharding import PartitionSpec as P

HEAD_WIDTH = 128
MASKED = -1e30
SCALE_LOG2 = HEAD_WIDTH ** (-0.5) * 1.4426950408889634
MESH = pl.DeviceIdType.MESH
ROW_TILE = 256


def fused(
    sizes,
    half_ref,
    frame_ref,
    q_hbm,
    k_hbm,
    v_hbm,
    w_hbm,
    res_hbm,
    gain_hbm,
    att_hbm,
    hid_hbm,
    norm_hbm,
    q_buf,
    qaug,
    kv,
    kaug,
    vaug,
    m_buf,
    acc,
    attf,
    wbuf,
    c_out,
    c_in,
    res_buf,
    gain_buf,
    hid_buf,
    norm_buf,
    e_out,
    e_in,
    io_sem,
    kz_s,
    kz_r,
    ks_s,
    ks_r,
    wz_s,
    w_r,
    wy_s,
    c_s,
    c_r,
    a_s,
    a_r,
    e_s,
    e_r,
):
    G, S, H, C = sizes
    use_y = G % 2 == 0
    half = S // 2
    per = S // H
    T = q_buf.shape[0]
    K = wbuf.shape[1]
    heads = q_buf.shape[1] // HEAD_WIDTH
    hb = T // 2
    g, s, h, c = (lax.axis_index(a) for a in ("groups", "seq", "heads", "sub"))
    right, left = lax.rem(s + 1, S), lax.rem(s + S - 1, S)
    other = 1 - c

    ins = [
        pltpu.make_async_copy(k_hbm, kv.at[0, 0, 0], io_sem.at[0]),
        pltpu.make_async_copy(v_hbm, kv.at[0, 0, 1], io_sem.at[1]),
        pltpu.make_async_copy(q_hbm, q_buf, io_sem.at[2]),
        pltpu.make_async_copy(w_hbm, wbuf.at[0], io_sem.at[3]),
        pltpu.make_async_copy(res_hbm, res_buf, io_sem.at[4]),
        pltpu.make_async_copy(gain_hbm, gain_buf, io_sem.at[5]),
    ]
    for copy in ins:
        copy.start()

    barrier = pltpu.get_barrier_semaphore()
    peers = [{"seq": left}, {"seq": right}, {"sub": other}]
    if use_y:
        parity = lax.rem(g, 2)
        partner = g + 1 - 2 * parity
        peers.append({"groups": partner})
    for i in range(1, H):
        to = lax.rem(h + i, H)
        peers.append({"heads": to})
        peers.append({"heads": to, "sub": other})
    for peer in peers:
        pl.semaphore_signal(barrier, inc=1, device_id=peer, device_id_type=MESH)

    if use_y:
        part = K * 5 // 16
        first = pl.ds(pl.multiple_of(parity * (K - part), 16), part)
        second = pl.ds(part, K - 2 * part)
        third = pl.ds(pl.multiple_of((1 - parity) * (K - part), 16), part)
        first_at = pl.multiple_of(parity * (K - part), 16)
    else:
        part = K // 2
        first = pl.ds(0, part)
        second = pl.ds(part, K - part)
        third = None
        first_at = 0
    second_rows = K - 2 * part if use_y else K - part
    pieces = half // 2

    def remote(src, dst, send, recv, device):
        return pltpu.make_async_remote_copy(
            src_ref=src, dst_ref=dst, send_sem=send, recv_sem=recv, device_id=device, device_id_type=MESH
        )

    def got(ref, sem):
        remote(ref, ref, a_s, sem, {"sub": other}).wait_recv()

    def sent(ref, sem):
        remote(ref, ref, sem, a_r, {"sub": other}).wait_send()

    def key_right(d, i):
        remote(kv.at[0, d, i], kv.at[0, d + 1, i], kz_s.at[0, d, i], kz_r.at[d + 1, i], {"seq": right}).start()

    def key_left(d, i):
        at = lax.rem(S - d, S)
        remote(kv.at[0, at, i], kv.at[0, S - d - 1, i], kz_s.at[1, d, i], kz_r.at[S - d - 1, i], {"seq": left}).start()

    def key_across(j):
        remote(kv.at[0, j], kv.at[1, j], ks_s.at[j], ks_r.at[j], {"sub": other}).start()

    def own_w(d):
        def send(at, rows, sub):
            ds = pl.ds(pl.multiple_of(at, 16), rows)
            remote(wbuf.at[0, ds], wbuf.at[1, ds], wz_s.at[0, 0, sub], w_r.at[1, sub], {"seq": right}).start()
            remote(wbuf.at[0, ds], wbuf.at[S - 1, ds], wz_s.at[1, 0, sub], w_r.at[S - 1, sub], {"seq": left}).start()

        @pl.when(d < pieces)
        def _():
            send(first_at + d * (part // pieces), part // pieces, 0)

        @pl.when(d >= pieces)
        def _():
            send(part + (d - pieces) * (second_rows // pieces), second_rows // pieces, 1)

    def w_right(d, rows, sub):
        remote(wbuf.at[d, rows], wbuf.at[d + 1, rows], wz_s.at[0, d, sub], w_r.at[d + 1, sub], {"seq": right}).start()

    def w_left(d, rows, sub):
        remote(
            wbuf.at[S - d, rows], wbuf.at[S - d - 1, rows], wz_s.at[1, d, sub], w_r.at[S - d - 1, sub], {"seq": left}
        ).start()

    def w_pair(j):
        if use_y:
            remote(wbuf.at[j, first], wbuf.at[j, first], wy_s.at[j], w_r.at[j, 2], {"groups": partner}).start()

    def w_pair_got(j):
        if use_y:
            got(wbuf.at[j, third], w_r.at[j, 2])

    lane = lax.broadcasted_iota(jnp.int32, (8, T), 1)
    own = (s * C + c) * 2
    position = jnp.where(lane < hb, half_ref[own] * hb + lane, half_ref[own + 1] * hb + lane - hb)
    limit = jnp.zeros((8, T), jnp.int32)
    start = jnp.int32(0)
    for f in range(frame_ref.shape[0]):
        length = frame_ref[f]
        limit = limit + jnp.where(start <= position, length, 0)
        start = start + length
    limit = jnp.broadcast_to(limit[0:1], (T, T))
    row = lax.broadcasted_iota(jnp.int32, (T, T), 0)
    col = lax.broadcasted_iota(jnp.int32, (T, T), 1)
    eye = jnp.where(row == col, 1.0, 0.0).astype(jnp.bfloat16)
    vaug[:, HEAD_WIDTH:] = jnp.ones((vaug.shape[0], HEAD_WIDTH), jnp.bfloat16)

    def place(at, which, j):
        block = (lax.rem(s - j + S, S) * C + (c if which == 0 else other)) * 2
        place_at = jnp.where(row < hb, half_ref[block] * hb + row, half_ref[block + 1] * hb + row - hb)
        hidden = jnp.where(place_at < limit, 0.0, MASKED).astype(jnp.bfloat16)
        kaug[at * T : (at + 1) * T, :HEAD_WIDTH] = kv[which, j, 0]
        kaug[at * T : (at + 1) * T, HEAD_WIDTH:] = hidden
        vaug[at * T : (at + 1) * T, :HEAD_WIDTH] = kv[which, j, 1]

    def attend(slots, opening=False):
        for at, j in enumerate(slots):
            place(2 * at, 0, j)
            got(kv.at[1, j], ks_r.at[j])
            place(2 * at + 1, 1, j)
        count = 2 * len(slots) * T

        def rows_of(i, carry):
            rows = pl.ds(pl.multiple_of(i * ROW_TILE, ROW_TILE), ROW_TILE)
            scores = lax.dot_general(
                qaug[rows], kaug[:count], (((1,), (1,)), ((), ())), preferred_element_type=jnp.float32
            )
            top = jnp.max(scores, axis=1, keepdims=True)
            if opening:
                new = jnp.broadcast_to(top, (ROW_TILE, HEAD_WIDTH))
            else:
                old = m_buf[rows]
                new = jnp.maximum(old, top)
            m_buf[rows] = new
            weights = jnp.exp2((scores - jnp.concatenate([new] * (count // HEAD_WIDTH), axis=1)) * SCALE_LOG2)
            product = jnp.dot(weights.astype(jnp.bfloat16), vaug[:count], preferred_element_type=jnp.float32)
            if opening:
                acc[rows] = product
            else:
                fade = jnp.exp2((old - new) * SCALE_LOG2)
                acc[rows] = acc[rows] * jnp.concatenate([fade, fade], axis=1) + product
            return carry

        lax.fori_loop(0, heads * T // ROW_TILE, rows_of, 0)

    pl.semaphore_wait(barrier, len(peers))
    ins[0].wait()
    key_right(0, 0)
    key_left(0, 0)
    ins[1].wait()
    key_right(0, 1)
    key_left(0, 1)
    key_across(0)
    ins[3].wait()
    own_w(0)
    ins[2].wait()
    for i in range(heads):
        qaug[i * T : (i + 1) * T, :HEAD_WIDTH] = q_buf[:, i * HEAD_WIDTH : (i + 1) * HEAD_WIDTH]
        qaug[i * T : (i + 1) * T, HEAD_WIDTH:] = eye

    def key_round(d, last):
        for i in range(2):
            got(kv.at[0, d, i], kz_r.at[d, i])
            if not last or i == 0:
                key_right(d, i)
            got(kv.at[0, S - d, i], kz_r.at[S - d, i])
            if not last or i == 1:
                key_left(d, i)
        key_across(d)
        key_across(S - d)
        own_w(d)

    key_round(1, half == 2)
    attend([0], opening=True)

    def key_step(d, carry):
        key_round(d, False)
        attend([d - 1, S - d + 1])
        return carry

    lax.fori_loop(2, half - 1, key_step, 0)
    if half > 2:
        key_round(half - 1, True)
        attend([half - 2, S - half + 2])
    got(kv.at[0, half, 0], kz_r.at[half, 0])
    got(kv.at[0, half, 1], kz_r.at[half, 1])
    key_across(half)
    attend([half - 1, S - half + 1])

    def w_first(d, last):
        got(wbuf.at[d, first], w_r.at[d, 0])
        w_right(d, first, 0)
        w_pair(d)
        got(wbuf.at[S - d, first], w_r.at[S - d, 0])
        if not last:
            w_left(d, first, 0)
        w_pair(S - d)

    def w_second(d, last):
        got(wbuf.at[d, second], w_r.at[d, 1])
        if not last:
            w_right(d, second, 1)
        got(wbuf.at[S - d, second], w_r.at[S - d, 1])
        w_left(d, second, 1)

    w_first(1, half == 2)
    attend([half])
    w_second(1, half == 2)
    for i in range(heads):
        rows = slice(i * T, (i + 1) * T)
        cols = slice(i * HEAD_WIDTH, (i + 1) * HEAD_WIDTH)
        attf[0, :, cols] = (acc[rows, :HEAD_WIDTH] / acc[rows, HEAD_WIDTH:]).astype(jnp.bfloat16)
    across = remote(attf.at[0], attf.at[1], a_s, a_r, {"sub": other})
    across.start()
    att_copy = pltpu.make_async_copy(attf.at[0], att_hbm, io_sem.at[6])
    att_copy.start()

    def route(j):
        block = lax.rem(s - j + S, S)
        return block // per, lax.rem(block, per) * C + c

    def own_route(j, to, tile):
        return remote(c_out.at[j, 0], c_in.at[h, tile], c_s.at[j, 0], c_r.at[h, tile], {"heads": to})

    def project(slots):
        both = jnp.concatenate([attf[0], attf[1]], axis=0)
        weights = jnp.concatenate([wbuf[j] for j in slots], axis=1)
        terms = jnp.dot(both, weights, preferred_element_type=jnp.float32).astype(jnp.bfloat16)
        for i, j in enumerate(slots):
            for t in range(2):
                c_out[j, t] = terms[t * T : (t + 1) * T, i * T : (i + 1) * T]
        for j in slots:
            to, tile = route(j)
            remote(
                c_out.at[j, 1], c_in.at[h, tile], c_s.at[j, 1], c_r.at[h, tile], {"heads": to, "sub": other}
            ).start()

            @pl.when(to != h)
            def _():
                own_route(j, to, tile).start()

            @pl.when(to == h)
            def _():
                pltpu.make_async_copy(c_out.at[j, 0], c_in.at[h, tile], c_r.at[h, tile]).start()

    def w_step(d, carry):
        w_first(d, False)
        w_pair_got(d - 1)
        w_pair_got(S - d + 1)
        project([d - 1, S - d + 1])
        w_second(d, False)
        return carry

    if half > 2:
        w_first(2, half == 3)
        across.wait()
        project([0])
        w_second(2, half == 3)
        w_pair_got(1)
        w_pair_got(S - 1)
        project([1, S - 1])
        lax.fori_loop(3, half - 1, w_step, 0)
        w_first(half - 1, True)
        w_pair_got(half - 2)
        w_pair_got(S - half + 2)
        project([half - 2, S - half + 2])
        w_second(half - 1, True)
    else:
        across.wait()
        project([0])
    got(wbuf.at[half, first], w_r.at[half, 0])
    w_pair(half)
    w_pair_got(half - 1)
    w_pair_got(S - half + 1)
    project([half - 1, S - half + 1])
    got(wbuf.at[half, second], w_r.at[half, 1])
    w_pair_got(half)
    project([half])

    ins[4].wait()
    ins[5].wait()

    energy = jnp.zeros((T, 1), jnp.float32)
    tiles = c_in.shape[1]
    for t in range(tiles):
        cols = slice(t * T, (t + 1) * T)
        total = res_buf[:, cols].astype(jnp.float32)
        for p in range(H):
            got(c_in.at[p, t], c_r.at[p, t])
        summed = c_in[0, t].astype(jnp.float32)
        for p in range(1, H):
            summed = summed + c_in[p, t].astype(jnp.float32)
        state = (total + summed).astype(jnp.bfloat16)
        hid_buf[:, cols] = state
        wide = state.astype(jnp.float32)
        energy = energy + jnp.sum(wide * wide, axis=1, keepdims=True)
    e_out[...] = jnp.transpose(jnp.broadcast_to(energy, (T, T)))[:8]
    for i in range(1, H):
        to = lax.rem(h + i, H)
        remote(e_out, e_in.at[h], e_s.at[i], e_r.at[h], {"heads": to}).start()
    hid_copy = pltpu.make_async_copy(hid_buf, hid_hbm, io_sem.at[7])
    hid_copy.start()
    everyone = e_out[...]
    for i in range(1, H):
        of = lax.rem(h + i, H)
        got(e_in.at[of], e_r.at[of])
        everyone = everyone + e_in[of]
    mean = jnp.transpose(jnp.broadcast_to(everyone[0:1], (T, T))) * (1.0 / (T * tiles * H))
    factor = lax.rsqrt(mean + 1e-6)
    for t in range(tiles):
        cols = slice(t * T, (t + 1) * T)
        norm_buf[:, cols] = (hid_buf[:, cols].astype(jnp.float32) * factor * gain_buf[:, cols]).astype(jnp.bfloat16)
    norm_copy = pltpu.make_async_copy(norm_buf, norm_hbm, io_sem.at[8])
    norm_copy.start()

    def drain_keys(d, carry):
        for i in range(2):
            for way in range(2):
                sent(kv.at[0, 0, i], kz_s.at[way, d, i])
        return carry

    lax.fori_loop(0, half - 1, drain_keys, 0)
    sent(kv.at[0, 0, 0], kz_s.at[0, half - 1, 0])
    sent(kv.at[0, 0, 1], kz_s.at[1, half - 1, 1])

    def drain_w(d, carry):
        for way in range(2):
            sent(wbuf.at[0, first], wz_s.at[way, d, 0])
            sent(wbuf.at[0, second], wz_s.at[way, d, 1])
        return carry

    lax.fori_loop(0, half - 1, drain_w, 0)
    sent(wbuf.at[0, first], wz_s.at[0, half - 1, 0])
    sent(wbuf.at[0, second], wz_s.at[1, half - 1, 1])

    def drain_slots(j, carry):
        sent(kv.at[0, 0], ks_s.at[j])
        sent(c_out.at[0, 1], c_s.at[j, 1])
        to, tile = route(j)

        @pl.when(to != h)
        def _():
            sent(c_out.at[0, 0], c_s.at[j, 0])

        if use_y:

            @pl.when(j > 0)
            def _():
                sent(wbuf.at[0, first], wy_s.at[j])

        return carry

    lax.fori_loop(0, S, drain_slots, 0)
    for i in range(1, H):
        sent(e_out, e_s.at[i])
    att_copy.wait()
    hid_copy.wait()
    norm_copy.wait()


def shards(sizes, queries, keys, values, half_order, frame_lengths, out_proj, residual_in, norm_gain):
    G, S, H, C = sizes
    T, width = queries.shape
    K, cols = out_proj.shape
    tiles = residual_in.shape[1] // cols
    heads = width // HEAD_WIDTH
    bf16, f32, dma = jnp.bfloat16, jnp.float32, pltpu.SemaphoreType.DMA
    anywhere = pl.BlockSpec(memory_space=pl.ANY)
    smem = pl.BlockSpec(memory_space=pltpu.SMEM)
    return pl.pallas_call(
        functools.partial(fused, sizes),
        out_shape=(
            jax.ShapeDtypeStruct(queries.shape, bf16),
            jax.ShapeDtypeStruct(residual_in.shape, bf16),
            jax.ShapeDtypeStruct(residual_in.shape, bf16),
        ),
        in_specs=[smem, smem] + [anywhere] * 6,
        out_specs=(anywhere,) * 3,
        scratch_shapes=[
            pltpu.VMEM((T, width), bf16),
            pltpu.VMEM((heads * T, 2 * HEAD_WIDTH), bf16),
            pltpu.VMEM((2, S, 2, T, HEAD_WIDTH), bf16),
            pltpu.VMEM((4 * T, 2 * HEAD_WIDTH), bf16),
            pltpu.VMEM((4 * T, 2 * HEAD_WIDTH), bf16),
            pltpu.VMEM((heads * T, HEAD_WIDTH), f32),
            pltpu.VMEM((heads * T, 2 * HEAD_WIDTH), f32),
            pltpu.VMEM((2, T, width), bf16),
            pltpu.VMEM((S, K, cols), bf16),
            pltpu.VMEM((S, 2, T, cols), bf16),
            pltpu.VMEM((H, tiles, T, cols), bf16),
            pltpu.VMEM(residual_in.shape, bf16),
            pltpu.VMEM((1, residual_in.shape[1]), f32),
            pltpu.VMEM(residual_in.shape, bf16),
            pltpu.VMEM(residual_in.shape, bf16),
            pltpu.VMEM((8, T), f32),
            pltpu.VMEM((H, 8, T), f32),
            dma((9,)),
            dma((2, S // 2, 2)),
            dma((S, 2)),
            dma((S,)),
            dma((S,)),
            dma((2, S // 2, 2)),
            dma((S, 3)),
            dma((S,)),
            dma((S, 2)),
            dma((H, tiles)),
            dma(()),
            dma(()),
            dma((H,)),
            dma((H,)),
        ],
        compiler_params=pltpu.CompilerParams(collective_id=0, has_side_effects=True),
    )(half_order, frame_lengths, queries, keys, values, out_proj, residual_in, norm_gain.reshape(1, -1))


def solution(mesh):
    sizes = tuple(mesh.shape[a] for a in ("groups", "seq", "heads", "sub"))
    rows = P(("groups", "seq", "sub"), "heads")
    in_specs = (rows, rows, rows, P("groups"), P("groups"), P("heads", ("seq", "sub")), rows, P("heads"))
    return jax.shard_map(
        functools.partial(shards, sizes), mesh=mesh, in_specs=in_specs, out_specs=(rows,) * 3, check_vma=False
    )
```

```python
import functools

import jax
import jax.numpy as jnp
from jax import lax
from jax.experimental import pallas as pl
from jax.experimental.pallas import tpu as pltpu
from jax.sharding import PartitionSpec as P

HEAD_WIDTH = 128
MASKED = -1e30
SCALE_LOG2 = HEAD_WIDTH ** (-0.5) * 1.4426950408889634
MESH = pl.DeviceIdType.MESH
ROW_TILE = 512
LAG = 3
Y_ROWS = 5


def fused(
    sizes,
    half_ref,
    frame_ref,
    q_hbm,
    k_hbm,
    v_hbm,
    w_hbm,
    res_hbm,
    gain_hbm,
    att_hbm,
    hid_hbm,
    norm_hbm,
    q_buf,
    qaug,
    kv,
    kaug,
    vaug,
    m_buf,
    acc,
    attf,
    wbuf,
    c_out,
    c_in,
    res_buf,
    gain_buf,
    hid_buf,
    norm_buf,
    e_out,
    e_in,
    io_sem,
    line_sem,
    ring_sem,
    kz_s,
    kz_r,
    kd_s,
    ks_s,
    ks_r,
    wz_s,
    w_r,
    wd_s,
    wy_s,
    c_s,
    c_r,
    a_s,
    a_r,
    e_s,
    e_r,
):
    G, S, H, C = sizes
    use_y = G % 2 == 0
    half = S // 2
    lag = min(LAG, half - 1)
    per = S // H
    T = q_buf.shape[0]
    K = wbuf.shape[1]
    heads = q_buf.shape[1] // HEAD_WIDTH
    hb = T // 2
    g, s, h, c = (lax.axis_index(a) for a in ("groups", "seq", "heads", "sub"))
    right, left = lax.rem(s + 1, S), lax.rem(s + S - 1, S)
    h_up, h_down = lax.rem(h + 1, H), lax.rem(h + H - 1, H)
    other = 1 - c
    both, either = jnp.logical_and, jnp.logical_or

    ins = [
        pltpu.make_async_copy(k_hbm, kv.at[0, s, 0], io_sem.at[0]),
        pltpu.make_async_copy(v_hbm, kv.at[0, s, 1], io_sem.at[1]),
        pltpu.make_async_copy(q_hbm, q_buf, io_sem.at[2]),
        pltpu.make_async_copy(w_hbm, wbuf.at[s], io_sem.at[3]),
        pltpu.make_async_copy(res_hbm, res_buf, io_sem.at[4]),
        pltpu.make_async_copy(gain_hbm, gain_buf, io_sem.at[5]),
    ]
    for copy in ins:
        copy.start()

    barrier = pltpu.get_barrier_semaphore()

    def signal(sem, device):
        pl.semaphore_signal(sem, inc=1, device_id=device, device_id_type=MESH)

    signal(barrier, {"sub": other})
    signal(barrier, {"heads": h_up})
    signal(barrier, {"heads": h_down})
    greeted = 3
    if use_y:
        parity = lax.rem(g, 2)
        partner = g + 1 - 2 * parity
        signal(barrier, {"groups": partner})
        greeted = 4

    @pl.when(s > 0)
    def _():
        signal(barrier, {"seq": s - 1})

    @pl.when(s < S - 1)
    def _():
        signal(barrier, {"seq": s + 1})

    if use_y:
        part = K * Y_ROWS // 16
        first = pl.ds(pl.multiple_of(parity * (K - part), 16), part)
        second = pl.ds(part, K - 2 * part)
        third = pl.ds(pl.multiple_of((1 - parity) * (K - part), 16), part)
    else:
        part = K // 2
        first = pl.ds(0, part)
        second = pl.ds(part, K - part)
        third = None

    def remote(src, dst, send, recv, device):
        return pltpu.make_async_remote_copy(
            src_ref=src, dst_ref=dst, send_sem=send, recv_sem=recv, device_id=device, device_id_type=MESH
        )

    def got(ref, sem):
        remote(ref, ref, a_s, sem, {"sub": other}).wait_recv()

    def sent(ref, sem):
        remote(ref, ref, sem, a_r, {"sub": other}).wait_send()

    def left_needs(j):
        return either(both(s > 0, both(j >= s, j - s < half)), left - j > half)

    def right_needs(j):
        return both(s < S - 1, either(both(j <= s, s - j < half), j - s - 1 > half))

    def key_send(j, i, way):
        to = right if way else left
        remote(kv.at[0, j, i], kv.at[0, j, i], kz_s.at[way, j, i], kz_r.at[j, i], {"seq": to}).start()

    def key_direct(i):
        remote(kv.at[0, s, i], kv.at[0, s, i], kd_s.at[i], kz_r.at[s, i], {"seq": 0}).start()

    def key_across(j):
        remote(kv.at[0, j], kv.at[1, j], ks_s.at[j], ks_r.at[j], {"sub": other}).start()

    def w_send(j, i, way):
        rows = second if i else first
        to = right if way else left
        remote(wbuf.at[j, rows], wbuf.at[j, rows], wz_s.at[way, j, i], w_r.at[j, i], {"seq": to}).start()

    def w_direct(i):
        rows = second if i else first
        remote(wbuf.at[s, rows], wbuf.at[s, rows], wd_s.at[i], w_r.at[s, i], {"seq": 0}).start()

    lane = lax.broadcasted_iota(jnp.int32, (8, T), 1)
    own = (s * C + c) * 2
    position = jnp.where(lane < hb, half_ref[own] * hb + lane, half_ref[own + 1] * hb + lane - hb)
    limit = jnp.zeros((8, T), jnp.int32)
    start = jnp.int32(0)
    for f in range(frame_ref.shape[0]):
        length = frame_ref[f]
        limit = limit + jnp.where(start <= position, length, 0)
        start = start + length
    limit = jnp.broadcast_to(limit[0:1], (T, T))
    row = lax.broadcasted_iota(jnp.int32, (T, T), 0)
    col = lax.broadcasted_iota(jnp.int32, (T, T), 1)
    eye = jnp.where(row == col, 1.0, 0.0).astype(jnp.bfloat16)
    vaug[:, HEAD_WIDTH:] = jnp.ones((vaug.shape[0], HEAD_WIDTH), jnp.bfloat16)

    def place(at, which, j):
        block = (j * C + (c if which == 0 else other)) * 2
        place_at = jnp.where(row < hb, half_ref[block] * hb + row, half_ref[block + 1] * hb + row - hb)
        hidden = jnp.where(place_at < limit, 0.0, MASKED).astype(jnp.bfloat16)
        kaug[at * T : (at + 1) * T, :HEAD_WIDTH] = kv[which, j, 0]
        kaug[at * T : (at + 1) * T, HEAD_WIDTH:] = hidden
        vaug[at * T : (at + 1) * T, :HEAD_WIDTH] = kv[which, j, 1]

    def attend(j, opening=False):
        place(0, 0, j)
        got(kv.at[1, j], ks_r.at[j])
        place(1, 1, j)
        tile = min(ROW_TILE, heads * T)

        def rows_of(i, carry):
            rows = pl.ds(pl.multiple_of(i * tile, tile), tile)
            scores = lax.dot_general(
                qaug[rows], kaug[...], (((1,), (1,)), ((), ())), preferred_element_type=jnp.float32
            )
            top = jnp.max(scores, axis=1, keepdims=True)
            if opening:
                new = jnp.broadcast_to(top, (tile, HEAD_WIDTH))
            else:
                old = m_buf[rows]
                new = jnp.maximum(old, top)
            m_buf[rows] = new
            weights = jnp.exp2((scores - jnp.concatenate([new, new], axis=1)) * SCALE_LOG2)
            product = jnp.dot(weights.astype(jnp.bfloat16), vaug[...], preferred_element_type=jnp.float32)
            if opening:
                acc[rows] = product
            else:
                fade = jnp.exp2((old - new) * SCALE_LOG2)
                acc[rows] = acc[rows] * jnp.concatenate([fade, fade], axis=1) + product
            return carry

        lax.fori_loop(0, heads * T // tile, rows_of, 0)

    pl.semaphore_wait(
        barrier, greeted + jnp.where(s > 0, 1, 0).astype(jnp.int32) + jnp.where(s < S - 1, 1, 0).astype(jnp.int32)
    )

    @pl.when(s > 0)
    def _():
        pl.semaphore_wait(line_sem, 1)

    @pl.when(s < S - 1)
    def _():
        signal(line_sem, {"seq": s + 1})

    def own_keys(i):
        @pl.when(s > 0)
        def _():
            key_send(s, i, 0)

        @pl.when(s < S - 1)
        def _():
            key_send(s, i, 1)

        @pl.when(s > half)
        def _():
            key_direct(i)

    def own_w(i):
        @pl.when(s > 0)
        def _():
            w_send(s, i, 0)

        @pl.when(s < S - 1)
        def _():
            w_send(s, i, 1)

        @pl.when(s > half)
        def _():
            w_direct(i)

    ins[0].wait()
    own_keys(0)
    ins[1].wait()
    own_keys(1)
    key_across(s)
    ins[3].wait()
    own_w(0)
    own_w(1)

    for r in range(H // 2):
        signal(ring_sem.at[0, r], {"heads": h_up})
        signal(ring_sem.at[1, r], {"heads": h_down})
        pl.semaphore_wait(ring_sem.at[0, r], 1)
        pl.semaphore_wait(ring_sem.at[1, r], 1)

    ins[2].wait()
    for i in range(heads):
        qaug[i * T : (i + 1) * T, :HEAD_WIDTH] = q_buf[:, i * HEAD_WIDTH : (i + 1) * HEAD_WIDTH]
        qaug[i * T : (i + 1) * T, HEAD_WIDTH:] = eye

    def key_take(j, onward):
        for i in range(2):
            got(kv.at[0, j, i], kz_r.at[j, i])
            onward(j, i)
        key_across(j)

    def w_take(j, onward):
        got(wbuf.at[j, first], w_r.at[j, 0])
        onward(j, 0)
        if use_y:
            remote(wbuf.at[j, first], wbuf.at[j, first], wy_s.at[j], w_r.at[j, 2], {"groups": partner}).start()
        got(wbuf.at[j, second], w_r.at[j, 1])
        onward(j, 1)

    def guarded(condition, send, way):
        def onward(j, i):
            @pl.when(condition(j))
            def _():
                send(j, i, way)

        return onward

    def lines(p, act):
        @pl.when(s + p < S)
        def _():
            act(s + p, 0)

        @pl.when(s - p >= 0)
        def _():
            act(s - p, 1)

    def key_line(p):
        go = (
            guarded(lambda j: both(s > 0, p < half), key_send, 0),
            guarded(lambda j: both(s < S - 1, p < half), key_send, 1),
        )
        lines(p, lambda j, way: key_take(j, go[way]))

    def w_line(p, late):
        if late:
            up = guarded(lambda j: either(both(s > 0, p < half), both(s == 0, j < S - 1 - half)), w_send, 0)
        else:
            up = guarded(lambda j: both(s > 0, p < half), w_send, 0)
        go = (up, guarded(lambda j: both(s < S - 1, p < half), w_send, 1))
        lines(p, lambda j, way: w_take(j, go[way]))

    def wraps(k, act):
        @pl.when(s + half + k < S)
        def _():
            act(s + half + k, 1)

        @pl.when(k <= s - half)
        def _():
            act(k - 1, 0)

    def key_wrap(k):
        go = (
            guarded(lambda j: s - 1 - j > half, key_send, 0),
            guarded(lambda j: j - s - 1 > half, key_send, 1),
        )
        wraps(k, lambda j, way: key_take(j, go[way]))

    def w_wrap(k):
        go = (
            guarded(lambda j: s - 1 - j > half, w_send, 0),
            guarded(lambda j: j - s - 1 > half, w_send, 1),
        )
        wraps(k, lambda j, way: w_take(j, go[way]))

    def attend_line(p):
        lines(p, lambda j, way: attend(j))

    key_line(1)
    attend(s, opening=True)

    def line_step(p, carry):
        key_line(p)
        attend_line(p - 1)

        @pl.when(p > lag)
        def _():
            w_line(p - lag, False)

        return carry

    lax.fori_loop(2, half + 1, line_step, 0)
    attend_line(half)

    def wrap_step(k, carry):
        key_wrap(k)
        wraps(k, lambda j, way: attend(j))
        return carry

    lax.fori_loop(1, half, wrap_step, 0)

    @pl.when(s == 0)
    def _():
        def keys_round(j, carry):
            key_send(j, 0, 0)
            key_send(j, 1, 0)
            return carry

        lax.fori_loop(0, S - 1 - half, keys_round, 0)

        def w_round(j, carry):
            w_send(j, 0, 0)
            w_send(j, 1, 0)
            return carry

        lax.fori_loop(0, min(S - 1 - half, half - lag + 1), w_round, 0)

    for i in range(heads):
        rows = slice(i * T, (i + 1) * T)
        cols = slice(i * HEAD_WIDTH, (i + 1) * HEAD_WIDTH)
        attf[0, :, cols] = (acc[rows, :HEAD_WIDTH] / acc[rows, HEAD_WIDTH:]).astype(jnp.bfloat16)
    across = remote(attf.at[0], attf.at[1], a_s, a_r, {"sub": other})
    across.start()
    att_copy = pltpu.make_async_copy(attf.at[0], att_hbm, io_sem.at[6])
    att_copy.start()

    def route(j):
        return j // per, lax.rem(j, per) * C + c

    def own_route(j, to, tile):
        return remote(c_out.at[j, 0], c_in.at[h, tile], c_s.at[j, 0], c_r.at[h, tile], {"heads": to})

    def project(j):
        if use_y:

            @pl.when(j != s)
            def _():
                got(wbuf.at[j, third], w_r.at[j, 2])

        rows = jnp.concatenate([attf[0], attf[1]], axis=0)
        terms = jnp.dot(rows, wbuf[j], preferred_element_type=jnp.float32).astype(jnp.bfloat16)
        for t in range(2):
            c_out[j, t] = terms[t * T : (t + 1) * T]
        to, tile = route(j)
        remote(
            c_out.at[j, 1], c_in.at[h, tile], c_s.at[j, 1], c_r.at[h, tile], {"heads": to, "sub": other}
        ).start()

        @pl.when(to != h)
        def _():
            own_route(j, to, tile).start()

        @pl.when(to == h)
        def _():
            pltpu.make_async_copy(c_out.at[j, 0], c_in.at[h, tile], c_r.at[h, tile]).start()

    def project_line(p):
        lines(p, lambda j, way: project(j))

    across.wait()
    project(s)

    def early_step(p, carry):
        project_line(p)
        return carry

    lax.fori_loop(1, half - lag, early_step, 0)

    def late_step(p, carry):
        w_line(p, True)
        project_line(p - 1)
        return carry

    if lag < half - 1:
        lax.fori_loop(half - lag + 1, half + 1, late_step, 0)
        project_line(half)
    else:
        lax.fori_loop(2, half + 1, late_step, 0)
        project_line(half)

    def wrap_late(k, carry):
        w_wrap(k)
        wraps(k, lambda j, way: project(j))
        return carry

    lax.fori_loop(1, half, wrap_late, 0)

    ins[4].wait()
    ins[5].wait()

    energy = jnp.zeros((T, 1), jnp.float32)
    tiles = c_in.shape[1]
    for t in range(tiles):
        cols = slice(t * T, (t + 1) * T)
        total = res_buf[:, cols].astype(jnp.float32)
        for p in range(H):
            got(c_in.at[p, t], c_r.at[p, t])
        summed = c_in[0, t].astype(jnp.float32)
        for p in range(1, H):
            summed = summed + c_in[p, t].astype(jnp.float32)
        state = (total + summed).astype(jnp.bfloat16)
        hid_buf[:, cols] = state
        wide = state.astype(jnp.float32)
        energy = energy + jnp.sum(wide * wide, axis=1, keepdims=True)
    e_out[...] = jnp.transpose(jnp.broadcast_to(energy, (T, T)))[:8]
    for i in range(1, H):
        to = lax.rem(h + i, H)
        remote(e_out, e_in.at[h], e_s.at[i], e_r.at[h], {"heads": to}).start()
    hid_copy = pltpu.make_async_copy(hid_buf, hid_hbm, io_sem.at[7])
    hid_copy.start()
    everyone = e_out[...]
    for i in range(1, H):
        of = lax.rem(h + i, H)
        got(e_in.at[of], e_r.at[of])
        everyone = everyone + e_in[of]
    mean = jnp.transpose(jnp.broadcast_to(everyone[0:1], (T, T))) * (1.0 / (T * tiles * H))
    factor = lax.rsqrt(mean + 1e-6)
    for t in range(tiles):
        cols = slice(t * T, (t + 1) * T)
        norm_buf[:, cols] = (hid_buf[:, cols].astype(jnp.float32) * factor * gain_buf[:, cols]).astype(jnp.bfloat16)
    norm_copy = pltpu.make_async_copy(norm_buf, norm_hbm, io_sem.at[8])
    norm_copy.start()

    def drain(j, carry):
        for way, needs in enumerate((left_needs, right_needs)):

            @pl.when(needs(j))
            def _(way=way):
                for i in range(2):
                    sent(kv.at[0, 0, i], kz_s.at[way, j, i])
                sent(wbuf.at[0, first], wz_s.at[way, j, 0])
                sent(wbuf.at[0, second], wz_s.at[way, j, 1])

        sent(kv.at[0, 0], ks_s.at[j])
        sent(c_out.at[0, 1], c_s.at[j, 1])
        to, tile = route(j)

        @pl.when(to != h)
        def _():
            sent(c_out.at[0, 0], c_s.at[j, 0])

        if use_y:

            @pl.when(j != s)
            def _():
                sent(wbuf.at[0, first], wy_s.at[j])

        return carry

    lax.fori_loop(0, S, drain, 0)

    @pl.when(s > half)
    def _():
        for i in range(2):
            sent(kv.at[0, 0, i], kd_s.at[i])
        sent(wbuf.at[0, first], wd_s.at[0])
        sent(wbuf.at[0, second], wd_s.at[1])

    for i in range(1, H):
        sent(e_out, e_s.at[i])
    att_copy.wait()
    hid_copy.wait()
    norm_copy.wait()


def shards(sizes, queries, keys, values, half_order, frame_lengths, out_proj, residual_in, norm_gain):
    G, S, H, C = sizes
    T, width = queries.shape
    K, cols = out_proj.shape
    tiles = residual_in.shape[1] // cols
    heads = width // HEAD_WIDTH
    bf16, f32, dma = jnp.bfloat16, jnp.float32, pltpu.SemaphoreType.DMA
    anywhere = pl.BlockSpec(memory_space=pl.ANY)
    smem = pl.BlockSpec(memory_space=pltpu.SMEM)
    return pl.pallas_call(
        functools.partial(fused, sizes),
        out_shape=(
            jax.ShapeDtypeStruct(queries.shape, bf16),
            jax.ShapeDtypeStruct(residual_in.shape, bf16),
            jax.ShapeDtypeStruct(residual_in.shape, bf16),
        ),
        in_specs=[smem, smem] + [anywhere] * 6,
        out_specs=(anywhere,) * 3,
        scratch_shapes=[
            pltpu.VMEM((T, width), bf16),
            pltpu.VMEM((heads * T, 2 * HEAD_WIDTH), bf16),
            pltpu.VMEM((2, S, 2, T, HEAD_WIDTH), bf16),
            pltpu.VMEM((2 * T, 2 * HEAD_WIDTH), bf16),
            pltpu.VMEM((2 * T, 2 * HEAD_WIDTH), bf16),
            pltpu.VMEM((heads * T, HEAD_WIDTH), f32),
            pltpu.VMEM((heads * T, 2 * HEAD_WIDTH), f32),
            pltpu.VMEM((2, T, width), bf16),
            pltpu.VMEM((S, K, cols), bf16),
            pltpu.VMEM((S, 2, T, cols), bf16),
            pltpu.VMEM((H, tiles, T, cols), bf16),
            pltpu.VMEM(residual_in.shape, bf16),
            pltpu.VMEM((1, residual_in.shape[1]), f32),
            pltpu.VMEM(residual_in.shape, bf16),
            pltpu.VMEM(residual_in.shape, bf16),
            pltpu.VMEM((8, T), f32),
            pltpu.VMEM((H, 8, T), f32),
            dma((9,)),
            pltpu.SemaphoreType.REGULAR,
            pltpu.SemaphoreType.REGULAR((2, H // 2)),
            dma((2, S, 2)),
            dma((S, 2)),
            dma((2,)),
            dma((S,)),
            dma((S,)),
            dma((2, S, 2)),
            dma((S, 3)),
            dma((2,)),
            dma((S,)),
            dma((S, 2)),
            dma((H, tiles)),
            dma(()),
            dma(()),
            dma((H,)),
            dma((H,)),
        ],
        compiler_params=pltpu.CompilerParams(collective_id=0, has_side_effects=True),
    )(half_order, frame_lengths, queries, keys, values, out_proj, residual_in, norm_gain.reshape(1, -1))


def solution(mesh):
    sizes = tuple(mesh.shape[a] for a in ("groups", "seq", "heads", "sub"))
    rows = P(("groups", "seq", "sub"), "heads")
    in_specs = (rows, rows, rows, P("groups"), P("groups"), P("heads", ("seq", "sub")), rows, P("heads"))
    return jax.shard_map(
        functools.partial(shards, sizes), mesh=mesh, in_specs=in_specs, out_specs=(rows,) * 3, check_vma=False
    )
```

```python
import functools

import jax
import jax.numpy as jnp
from jax import lax
from jax.experimental import pallas as pl
from jax.experimental.pallas import tpu as pltpu
from jax.sharding import PartitionSpec as P

HEAD_WIDTH = 128
MASKED = -1e30
SCALE_LOG2 = HEAD_WIDTH ** (-0.5) * 1.4426950408889634
MESH = pl.DeviceIdType.MESH
ROW_TILE = 256
Y_ROWS = 7
LAG = 4


def fused(
    sizes,
    half_ref,
    frame_ref,
    q_hbm,
    k_hbm,
    v_hbm,
    w_hbm,
    res_hbm,
    att_hbm,
    hid_hbm,
    sum_hbm,
    q_buf,
    qaug,
    kv,
    kaug,
    vaug,
    m_buf,
    acc,
    attf,
    wbuf,
    c_out,
    c_in,
    res_buf,
    hid_buf,
    e_out,
    e_in,
    e_sum,
    io_sem,
    ring_sem,
    kz_s,
    kz_r,
    ks_s,
    ks_r,
    wz_s,
    w_r,
    wy_s,
    c_s,
    c_r,
    a_s,
    a_r,
    e_s,
    e_r,
):
    G, S, H, C = sizes
    use_y = G % 2 == 0
    half = S // 2
    lag = max(1, half * LAG // 8)
    per = S // H
    T = q_buf.shape[0]
    K = wbuf.shape[1]
    heads = q_buf.shape[1] // HEAD_WIDTH
    hb = T // 2
    g, s, h, c = (lax.axis_index(a) for a in ("groups", "seq", "heads", "sub"))
    right, left = lax.rem(s + 1, S), lax.rem(s + S - 1, S)
    other = 1 - c

    ins = [
        pltpu.make_async_copy(k_hbm, kv.at[0, 0, 0], io_sem.at[0]),
        pltpu.make_async_copy(v_hbm, kv.at[0, 0, 1], io_sem.at[1]),
        pltpu.make_async_copy(q_hbm, q_buf, io_sem.at[2]),
        pltpu.make_async_copy(w_hbm, wbuf.at[0], io_sem.at[3]),
        pltpu.make_async_copy(res_hbm, res_buf, io_sem.at[4]),
    ]
    for copy in ins:
        copy.start()

    barrier = pltpu.get_barrier_semaphore()
    peers = [{"seq": left}, {"seq": right}, {"sub": other}]
    if use_y:
        parity = lax.rem(g, 2)
        partner = g + 1 - 2 * parity
        peers.append({"groups": partner})
    h_up, h_down = lax.rem(h + 1, H), lax.rem(h + H - 1, H)
    peers += [{"heads": h_up}, {"heads": h_down}]
    for peer in peers:
        pl.semaphore_signal(barrier, inc=1, device_id=peer, device_id_type=MESH)

    if use_y:
        part = K * Y_ROWS // 16
        first = pl.ds(pl.multiple_of(parity * (K - part), 16), part)
        second = pl.ds(part, K - 2 * part)
        third = pl.ds(pl.multiple_of((1 - parity) * (K - part), 16), part)
        first_at = pl.multiple_of(parity * (K - part), 16)
    else:
        part = K // 2
        first = pl.ds(0, part)
        second = pl.ds(part, K - part)
        third = None
        first_at = 0
    second_rows = K - 2 * part if use_y else K - part
    pieces = max(1, half // 4)

    def remote(src, dst, send, recv, device):
        return pltpu.make_async_remote_copy(
            src_ref=src, dst_ref=dst, send_sem=send, recv_sem=recv, device_id=device, device_id_type=MESH
        )

    def got(ref, sem):
        remote(ref, ref, a_s, sem, {"sub": other}).wait_recv()

    def sent(ref, sem):
        remote(ref, ref, sem, a_r, {"sub": other}).wait_send()

    def key_right(d, i):
        remote(kv.at[0, d, i], kv.at[0, d + 1, i], kz_s.at[0, d, i], kz_r.at[d + 1, i], {"seq": right}).start()

    def key_left(d, i):
        at = lax.rem(S - d, S)
        remote(kv.at[0, at, i], kv.at[0, S - d - 1, i], kz_s.at[1, d, i], kz_r.at[S - d - 1, i], {"seq": left}).start()

    def key_across(j):
        remote(kv.at[0, j], kv.at[1, j], ks_s.at[j], ks_r.at[j], {"sub": other}).start()

    def own_w(d):
        def send(at, rows, sub):
            ds = pl.ds(pl.multiple_of(at, 16), rows)
            remote(wbuf.at[0, ds], wbuf.at[1, ds], wz_s.at[0, 0, sub], w_r.at[1, sub], {"seq": right}).start()
            remote(wbuf.at[0, ds], wbuf.at[S - 1, ds], wz_s.at[1, 0, sub], w_r.at[S - 1, sub], {"seq": left}).start()

        @pl.when(d < pieces)
        def _():
            send(first_at + d * (part // pieces), part // pieces, 0)

        @pl.when(jnp.logical_and(d >= pieces, d < 2 * pieces))
        def _():
            send(part + (d - pieces) * (second_rows // pieces), second_rows // pieces, 1)

    def w_right(d, rows, sub):
        remote(wbuf.at[d, rows], wbuf.at[d + 1, rows], wz_s.at[0, d, sub], w_r.at[d + 1, sub], {"seq": right}).start()

    def w_left(d, rows, sub):
        remote(
            wbuf.at[S - d, rows], wbuf.at[S - d - 1, rows], wz_s.at[1, d, sub], w_r.at[S - d - 1, sub], {"seq": left}
        ).start()

    def w_pair(j):
        if use_y:
            remote(wbuf.at[j, first], wbuf.at[j, first], wy_s.at[j], w_r.at[j, 2], {"groups": partner}).start()

    def w_pair_got(j):
        if use_y:
            got(wbuf.at[j, third], w_r.at[j, 2])

    lane = lax.broadcasted_iota(jnp.int32, (8, T), 1)
    own = (s * C + c) * 2
    position = jnp.where(lane < hb, half_ref[own] * hb + lane, half_ref[own + 1] * hb + lane - hb)
    limit = jnp.zeros((8, T), jnp.int32)
    start = jnp.int32(0)
    for f in range(frame_ref.shape[0]):
        length = frame_ref[f]
        limit = limit + jnp.where(start <= position, length, 0)
        start = start + length
    limit = jnp.broadcast_to(limit[0:1], (T, T))
    row = lax.broadcasted_iota(jnp.int32, (T, T), 0)
    col = lax.broadcasted_iota(jnp.int32, (T, T), 1)
    eye = jnp.where(row == col, 1.0, 0.0).astype(jnp.bfloat16)
    vaug[:, HEAD_WIDTH:] = jnp.ones((vaug.shape[0], HEAD_WIDTH), jnp.bfloat16)

    def place(at, which, j):
        block = (lax.rem(s - j + S, S) * C + (c if which == 0 else other)) * 2
        place_at = jnp.where(row < hb, half_ref[block] * hb + row, half_ref[block + 1] * hb + row - hb)
        hidden = jnp.where(place_at < limit, 0.0, MASKED).astype(jnp.bfloat16)
        kaug[at * T : (at + 1) * T, :HEAD_WIDTH] = kv[which, j, 0]
        kaug[at * T : (at + 1) * T, HEAD_WIDTH:] = hidden
        vaug[at * T : (at + 1) * T, :HEAD_WIDTH] = kv[which, j, 1]

    tile = min(ROW_TILE, heads * T)

    def prepare(slots):
        for at, j in enumerate(slots):
            place(2 * at, 0, j)
            got(kv.at[1, j], ks_r.at[j])
            place(2 * at + 1, 1, j)

    def attend_rows(slots, first_tile, last_tile, opening=False):
        count = 2 * len(slots) * T

        for i in range(first_tile, last_tile):
            rows = slice(i * tile, (i + 1) * tile)
            scores = lax.dot_general(
                qaug[rows], kaug[:count], (((1,), (1,)), ((), ())), preferred_element_type=jnp.float32
            )
            top = jnp.max(scores, axis=1, keepdims=True)
            if opening:
                new = jnp.broadcast_to(top, (tile, HEAD_WIDTH))
            else:
                old = m_buf[rows]
                new = jnp.maximum(old, top)
            m_buf[rows] = new
            weights = jnp.exp2((scores - jnp.concatenate([new] * (count // HEAD_WIDTH), axis=1)) * SCALE_LOG2)
            product = jnp.dot(weights.astype(jnp.bfloat16), vaug[:count], preferred_element_type=jnp.float32)
            if opening:
                acc[rows] = product
            else:
                fade = jnp.exp2((old - new) * SCALE_LOG2)
                acc[rows] = acc[rows] * jnp.concatenate([fade, fade], axis=1) + product

    row_tiles = heads * T // tile
    mid_tile = row_tiles // 2

    def attend(slots, opening=False, between=None):
        prepare(slots)
        attend_rows(slots, 0, mid_tile, opening)
        if between is not None:
            between()
        attend_rows(slots, mid_tile, row_tiles, opening)

    rounds = H // 2

    def ring_signal(r):
        pl.semaphore_signal(ring_sem.at[0, r], inc=1, device_id={"heads": h_up}, device_id_type=MESH)
        pl.semaphore_signal(ring_sem.at[1, r], inc=1, device_id={"heads": h_down}, device_id_type=MESH)

    def ring_wait(r):
        pl.semaphore_wait(ring_sem.at[0, r], 1)
        pl.semaphore_wait(ring_sem.at[1, r], 1)

    pl.semaphore_wait(barrier, len(peers))
    ins[0].wait()
    key_right(0, 0)
    key_left(0, 0)
    ins[1].wait()
    key_right(0, 1)
    key_left(0, 1)
    key_across(0)
    ins[3].wait()
    own_w(0)
    ring_signal(0)
    ins[2].wait()
    for i in range(heads):
        qaug[i * T : (i + 1) * T, :HEAD_WIDTH] = q_buf[:, i * HEAD_WIDTH : (i + 1) * HEAD_WIDTH]
        qaug[i * T : (i + 1) * T, HEAD_WIDTH:] = eye

    def key_round(d, last):
        for i in range(2):
            got(kv.at[0, d, i], kz_r.at[d, i])
            if not last or i == 0:
                key_right(d, i)
            got(kv.at[0, S - d, i], kz_r.at[S - d, i])
            if not last or i == 1:
                key_left(d, i)
        key_across(d)
        key_across(S - d)
        own_w(d)

    def w_first(d, last=False):
        got(wbuf.at[d, first], w_r.at[d, 0])
        w_right(d, first, 0)
        w_pair(d)
        got(wbuf.at[S - d, first], w_r.at[S - d, 0])
        if not last:
            w_left(d, first, 0)
        w_pair(S - d)

    def w_second(d, last=False):
        got(wbuf.at[d, second], w_r.at[d, 1])
        if not last:
            w_right(d, second, 1)
        got(wbuf.at[S - d, second], w_r.at[S - d, 1])
        w_left(d, second, 1)

    def finish():
        for i in range(heads):
            rows = slice(i * T, (i + 1) * T)
            cols = slice(i * HEAD_WIDTH, (i + 1) * HEAD_WIDTH)
            attf[0, :, cols] = (acc[rows, :HEAD_WIDTH] / acc[rows, HEAD_WIDTH:]).astype(jnp.bfloat16)

    across = remote(attf.at[0], attf.at[1], a_s, a_r, {"sub": other})
    att_copy = pltpu.make_async_copy(attf.at[0], att_hbm, io_sem.at[6])

    def route(j):
        block = lax.rem(s - j + S, S)
        to = block // per
        return to, lax.rem(block, per), lax.rem(to - h + H, H)

    def deliver(j):
        to, turn, away = route(j)
        tile = turn * C + c
        remote(
            c_out.at[j, 0], c_in.at[away, tile], c_s.at[j, 0], c_r.at[away, tile], {"heads": to}
        ).start()
        remote(
            c_out.at[j, 1], c_in.at[away, tile], c_s.at[j, 1], c_r.at[away, tile], {"heads": to, "sub": other}
        ).start()

    def project(slots):
        both = jnp.concatenate([attf[0], attf[1]], axis=0)
        weights = jnp.concatenate([wbuf[j] for j in slots], axis=1)
        terms = jnp.dot(both, weights, preferred_element_type=jnp.float32).astype(jnp.bfloat16)
        for i, j in enumerate(slots):
            for t in range(2):
                c_out[j, t] = terms[t * T : (t + 1) * T, i * T : (i + 1) * T]

    def send_sums(nearest, furthest):
        def owner(i, carry):
            for turn in range(per):
                block = lax.rem(h + i, H) * per + turn
                j = lax.rem(s - block + S, S)
                near = jnp.logical_and(j >= nearest, j <= furthest)
                beyond = jnp.logical_and(S - j >= nearest, S - j <= furthest)

                @pl.when(jnp.logical_or(near, beyond))
                def _(j=j, turn=turn):
                    @pl.when(i > 0)
                    def _():
                        deliver(j)

                    @pl.when(i == 0)
                    def _():
                        tile = turn * C + c
                        pltpu.make_async_copy(c_out.at[j, 0], c_in.at[0, tile], c_r.at[0, tile]).start()
                        remote(
                            c_out.at[j, 1], c_in.at[0, tile], c_s.at[j, 1], c_r.at[0, tile], {"sub": other}
                        ).start()

            return carry

        lax.fori_loop(0, H, owner, 0)

    key_round(1, half == 2)
    attend([0], opening=True)

    def key_step(d, carry):
        @pl.when(d - 2 < rounds)
        def _():
            ring_wait(d - 2)

        @pl.when(d - 1 < rounds)
        def _():
            ring_signal(d - 1)

        key_round(d, False)

        def between():
            @pl.when(d > lag)
            def _():
                w_first(d - lag)

        attend([d - 1, S - d + 1], between=between)

        @pl.when(d > lag)
        def _():
            w_second(d - lag)

        return carry

    if half > 2:
        lax.fori_loop(2, half - 1, key_step, 0)
        key_round(half - 1, True)
        attend([half - 2, S - half + 2], between=(lambda: w_first(half - 1 - lag)) if half - 1 > lag else None)
        if half - 1 > lag:
            w_second(half - 1 - lag)
    for r in range(max(0, half - 3), rounds):
        ring_wait(r)
        if r + 1 < rounds:
            ring_signal(r + 1)
    got(kv.at[0, half, 0], kz_r.at[half, 0])
    got(kv.at[0, half, 1], kz_r.at[half, 1])
    key_across(half)
    at = half - lag
    attend([half - 1, S - half + 1], between=lambda: w_first(at, at == half - 1))
    w_second(at, at == half - 1)

    def closing():
        attend([half])
        finish()
        across.start()
        att_copy.start()

    groups = [[0]] + [[d, S - d] for d in range(1, half)] + [[half]]
    done = 0

    def catch_up(upto):
        nonlocal done
        before = done
        while done < upto:
            for j in groups[done]:
                if j:
                    w_pair_got(j)
            project(groups[done])
            done += 1
        if done > before:
            send_sums(before, done - 1)

    todo = [closing, lambda: (across.wait(), catch_up(max(1, half - lag)))]
    for d in range(half - lag + 1, half):
        w_first(d, d == half - 1)
        if todo:
            todo.pop(0)()
        else:
            catch_up(d - 1)
        w_second(d, d == half - 1)
    got(wbuf.at[half, first], w_r.at[half, 0])
    w_pair(half)
    while todo:
        todo.pop(0)()
    catch_up(half)
    got(wbuf.at[half, second], w_r.at[half, 1])
    catch_up(half + 1)

    ins[4].wait()

    energy = jnp.zeros((T, 1), jnp.float32)
    tiles = c_in.shape[1]
    for t in range(tiles):
        cols = slice(t * T, (t + 1) * T)
        total = res_buf[:, cols].astype(jnp.float32)
        for p in range(H):
            got(c_in.at[p, t], c_r.at[p, t])
        summed = c_in[0, t].astype(jnp.float32)
        for p in range(1, H):
            summed = summed + c_in[p, t].astype(jnp.float32)
        state = (total + summed).astype(jnp.bfloat16)
        hid_buf[:, cols] = state
        wide = state.astype(jnp.float32)
        energy = energy + jnp.sum(wide * wide, axis=1, keepdims=True)
    e_out[...] = jnp.transpose(jnp.broadcast_to(energy, (T, T)))[:8]
    for i in range(1, H):
        to = lax.rem(h + i, H)
        remote(e_out, e_in.at[h], e_s.at[i], e_r.at[h], {"heads": to}).start()
    hid_copy = pltpu.make_async_copy(hid_buf, hid_hbm, io_sem.at[7])
    hid_copy.start()
    def drain_keys(d, carry):
        for i in range(2):
            for way in range(2):
                sent(kv.at[0, 0, i], kz_s.at[way, d, i])
        return carry

    lax.fori_loop(0, half - 1, drain_keys, 0)
    sent(kv.at[0, 0, 0], kz_s.at[0, half - 1, 0])
    sent(kv.at[0, 0, 1], kz_s.at[1, half - 1, 1])

    def drain_w(d, carry):
        for way in range(2):
            sent(wbuf.at[0, first], wz_s.at[way, d, 0])
            sent(wbuf.at[0, second], wz_s.at[way, d, 1])
        return carry

    lax.fori_loop(0, half - 1, drain_w, 0)
    sent(wbuf.at[0, first], wz_s.at[0, half - 1, 0])
    sent(wbuf.at[0, second], wz_s.at[1, half - 1, 1])

    def drain_slots(j, carry):
        sent(kv.at[0, 0], ks_s.at[j])
        away = route(j)[2]
        sent(c_out.at[0, 1], c_s.at[j, 1])

        @pl.when(away > 0)
        def _():
            sent(c_out.at[0, 0], c_s.at[j, 0])

        if use_y:

            @pl.when(j > 0)
            def _():
                sent(wbuf.at[0, first], wy_s.at[j])

        return carry

    lax.fori_loop(0, S, drain_slots, 0)
    everyone = e_out[...]
    for i in range(1, H):
        of = lax.rem(h + i, H)
        got(e_in.at[of], e_r.at[of])
        everyone = everyone + e_in[of]
    e_sum[...] = everyone
    sum_copy = pltpu.make_async_copy(e_sum, sum_hbm, io_sem.at[8])
    sum_copy.start()
    for i in range(1, H):
        sent(e_out, e_s.at[i])
    att_copy.wait()
    hid_copy.wait()
    sum_copy.wait()


def norm(width, sum_hbm, gain_hbm, att_hbm, hid_hbm, att_out, hid_out, norm_out, e_sum, gain, att, hid, normed, sems):
    T, cols = hid.shape
    pairs = ((att_hbm, att), (hid_hbm, hid), (sum_hbm, e_sum), (gain_hbm, gain))
    ins = [pltpu.make_async_copy(a, b, sems.at[i]) for i, (a, b) in enumerate(pairs)]
    for copy in ins:
        copy.start()
    outs = [
        pltpu.make_async_copy(a, b, sems.at[4 + i])
        for i, (a, b) in enumerate(((att, att_out), (hid, hid_out), (normed, norm_out)))
    ]
    ins[0].wait()
    outs[0].start()
    ins[1].wait()
    outs[1].start()
    ins[2].wait()
    ins[3].wait()
    mean = jnp.transpose(jnp.broadcast_to(e_sum[0:1], (T, T))) * (1.0 / width)
    factor = lax.rsqrt(mean + 1e-6)
    for t in range(cols // T):
        at = slice(t * T, (t + 1) * T)
        normed[:, at] = (hid[:, at].astype(jnp.float32) * factor * gain[:, at]).astype(jnp.bfloat16)
    outs[2].start()
    for copy in outs:
        copy.wait()


def shards(sizes, queries, keys, values, half_order, frame_lengths, out_proj, residual_in, norm_gain):
    G, S, H, C = sizes
    T, width = queries.shape
    K, cols = out_proj.shape
    tiles = residual_in.shape[1] // cols
    heads = width // HEAD_WIDTH
    bf16, f32, dma = jnp.bfloat16, jnp.float32, pltpu.SemaphoreType.DMA
    anywhere = pl.BlockSpec(memory_space=pl.ANY)
    smem = pl.BlockSpec(memory_space=pltpu.SMEM)
    attended, hidden, sums = pl.pallas_call(
        functools.partial(fused, sizes),
        out_shape=(
            jax.ShapeDtypeStruct(queries.shape, bf16),
            jax.ShapeDtypeStruct(residual_in.shape, bf16),
            jax.ShapeDtypeStruct((8, T), f32),
        ),
        in_specs=[smem, smem] + [anywhere] * 5,
        out_specs=(anywhere,) * 3,
        scratch_shapes=[
            pltpu.VMEM((T, width), bf16),
            pltpu.VMEM((heads * T, 2 * HEAD_WIDTH), bf16),
            pltpu.VMEM((2, S, 2, T, HEAD_WIDTH), bf16),
            pltpu.VMEM((4 * T, 2 * HEAD_WIDTH), bf16),
            pltpu.VMEM((4 * T, 2 * HEAD_WIDTH), bf16),
            pltpu.VMEM((heads * T, HEAD_WIDTH), f32),
            pltpu.VMEM((heads * T, 2 * HEAD_WIDTH), f32),
            pltpu.VMEM((2, T, width), bf16),
            pltpu.VMEM((S, K, cols), bf16),
            pltpu.VMEM((S, 2, T, cols), bf16),
            pltpu.VMEM((H, tiles, T, cols), bf16),
            pltpu.VMEM(residual_in.shape, bf16),
            pltpu.VMEM(residual_in.shape, bf16),
            pltpu.VMEM((8, T), f32),
            pltpu.VMEM((H, 8, T), f32),
            pltpu.VMEM((8, T), f32),
            dma((9,)),
            pltpu.SemaphoreType.REGULAR((2, H // 2)),
            dma((2, S // 2, 2)),
            dma((S, 2)),
            dma((S,)),
            dma((S,)),
            dma((2, S // 2, 2)),
            dma((S, 3)),
            dma((S,)),
            dma((S, 2)),
            dma((H, tiles)),
            dma(()),
            dma(()),
            dma((H,)),
            dma((H,)),
        ],
        compiler_params=pltpu.CompilerParams(collective_id=0, has_side_effects=True),
    )(half_order, frame_lengths, queries, keys, values, out_proj, residual_in)
    return pl.pallas_call(
        functools.partial(norm, residual_in.shape[1] * H),
        out_shape=(
            jax.ShapeDtypeStruct(queries.shape, bf16),
            jax.ShapeDtypeStruct(residual_in.shape, bf16),
            jax.ShapeDtypeStruct(residual_in.shape, bf16),
        ),
        in_specs=[anywhere] * 4,
        out_specs=(anywhere,) * 3,
        scratch_shapes=[
            pltpu.VMEM((8, T), f32),
            pltpu.VMEM((1, residual_in.shape[1]), f32),
            pltpu.VMEM((T, width), bf16),
            pltpu.VMEM(residual_in.shape, bf16),
            pltpu.VMEM(residual_in.shape, bf16),
            dma((7,)),
        ],
    )(sums, norm_gain.reshape(1, -1), attended, hidden)


def solution(mesh):
    sizes = tuple(mesh.shape[a] for a in ("groups", "seq", "heads", "sub"))
    rows = P(("groups", "seq", "sub"), "heads")
    in_specs = (rows, rows, rows, P("groups"), P("groups"), P("heads", ("seq", "sub")), rows, P("heads"))
    return jax.shard_map(
        functools.partial(shards, sizes), mesh=mesh, in_specs=in_specs, out_specs=(rows,) * 3, check_vma=False
    )
```

```python
import functools

import jax
import jax.numpy as jnp
from jax import lax
from jax.experimental import pallas as pl
from jax.experimental.pallas import tpu as pltpu
from jax.sharding import PartitionSpec as P

HEAD_WIDTH = 128
MASKED = -1e30
SCALE_LOG2 = HEAD_WIDTH ** (-0.5) * 1.4426950408889634
MESH = pl.DeviceIdType.MESH
ROW_TILE = 256
Y_ROWS = 6
LAG = 4


def fused(
    sizes,
    half_ref,
    frame_ref,
    q_hbm,
    k_hbm,
    v_hbm,
    w_hbm,
    res_hbm,
    att_hbm,
    hid_hbm,
    sum_hbm,
    q_buf,
    qaug,
    kv,
    kaug,
    vaug,
    m_buf,
    acc,
    attf,
    wbuf,
    c_out,
    c_in,
    m_in,
    m_far,
    res_buf,
    hid_buf,
    e_out,
    e_in,
    e_sum,
    io_sem,
    ring_sem,
    kz_s,
    kz_r,
    ks_s,
    ks_r,
    wz_s,
    w_r,
    wy_s,
    c_s,
    c_r,
    m_r,
    f_r,
    a_s,
    a_r,
    e_s,
    e_r,
):
    G, S, H, C = sizes
    use_y = G % 2 == 0
    half = S // 2
    lag = max(1, half * LAG // 8)
    per = S // H
    merging = H == 8
    T = q_buf.shape[0]
    K = wbuf.shape[1]
    heads = q_buf.shape[1] // HEAD_WIDTH
    hb = T // 2
    g, s, h, c = (lax.axis_index(a) for a in ("groups", "seq", "heads", "sub"))
    right, left = lax.rem(s + 1, S), lax.rem(s + S - 1, S)
    other = 1 - c

    ins = [
        pltpu.make_async_copy(k_hbm, kv.at[0, 0, 0], io_sem.at[0]),
        pltpu.make_async_copy(v_hbm, kv.at[0, 0, 1], io_sem.at[1]),
        pltpu.make_async_copy(q_hbm, q_buf, io_sem.at[2]),
        pltpu.make_async_copy(w_hbm, wbuf.at[0], io_sem.at[3]),
        pltpu.make_async_copy(res_hbm, res_buf, io_sem.at[4]),
    ]
    for copy in ins:
        copy.start()

    barrier = pltpu.get_barrier_semaphore()
    peers = [{"seq": left}, {"seq": right}, {"sub": other}]
    if use_y:
        parity = lax.rem(g, 2)
        partner = g + 1 - 2 * parity
        peers.append({"groups": partner})
    h_up, h_down = lax.rem(h + 1, H), lax.rem(h + H - 1, H)
    peers += [{"heads": h_up}, {"heads": h_down}]
    for peer in peers:
        pl.semaphore_signal(barrier, inc=1, device_id=peer, device_id_type=MESH)

    if use_y:
        part = K * Y_ROWS // 16
        first = pl.ds(pl.multiple_of(parity * (K - part), 16), part)
        second = pl.ds(part, K - 2 * part)
        third = pl.ds(pl.multiple_of((1 - parity) * (K - part), 16), part)
        first_at = pl.multiple_of(parity * (K - part), 16)
    else:
        part = K // 2
        first = pl.ds(0, part)
        second = pl.ds(part, K - part)
        third = None
        first_at = 0
    second_rows = K - 2 * part if use_y else K - part
    pieces = max(1, half // 4)

    def remote(src, dst, send, recv, device):
        return pltpu.make_async_remote_copy(
            src_ref=src, dst_ref=dst, send_sem=send, recv_sem=recv, device_id=device, device_id_type=MESH
        )

    def got(ref, sem):
        remote(ref, ref, a_s, sem, {"sub": other}).wait_recv()

    def sent(ref, sem):
        remote(ref, ref, sem, a_r, {"sub": other}).wait_send()

    def key_right(d, i):
        remote(kv.at[0, d, i], kv.at[0, d + 1, i], kz_s.at[0, d, i], kz_r.at[d + 1, i], {"seq": right}).start()

    def key_left(d, i):
        at = lax.rem(S - d, S)
        remote(kv.at[0, at, i], kv.at[0, S - d - 1, i], kz_s.at[1, d, i], kz_r.at[S - d - 1, i], {"seq": left}).start()

    def key_across(j):
        remote(kv.at[0, j], kv.at[1, j], ks_s.at[j], ks_r.at[j], {"sub": other}).start()

    def own_w(d):
        def send(at, rows, sub):
            ds = pl.ds(pl.multiple_of(at, 16), rows)
            remote(wbuf.at[0, ds], wbuf.at[1, ds], wz_s.at[0, 0, sub], w_r.at[1, sub], {"seq": right}).start()
            remote(wbuf.at[0, ds], wbuf.at[S - 1, ds], wz_s.at[1, 0, sub], w_r.at[S - 1, sub], {"seq": left}).start()

        @pl.when(d < pieces)
        def _():
            send(first_at + d * (part // pieces), part // pieces, 0)

        @pl.when(jnp.logical_and(d >= pieces, d < 2 * pieces))
        def _():
            send(part + (d - pieces) * (second_rows // pieces), second_rows // pieces, 1)

    def w_right(d, rows, sub):
        remote(wbuf.at[d, rows], wbuf.at[d + 1, rows], wz_s.at[0, d, sub], w_r.at[d + 1, sub], {"seq": right}).start()

    def w_left(d, rows, sub):
        remote(
            wbuf.at[S - d, rows], wbuf.at[S - d - 1, rows], wz_s.at[1, d, sub], w_r.at[S - d - 1, sub], {"seq": left}
        ).start()

    def w_pair(j):
        if use_y:
            remote(wbuf.at[j, first], wbuf.at[j, first], wy_s.at[j], w_r.at[j, 2], {"groups": partner}).start()

    def w_pair_got(j):
        if use_y:
            got(wbuf.at[j, third], w_r.at[j, 2])

    lane = lax.broadcasted_iota(jnp.int32, (8, T), 1)
    own = (s * C + c) * 2
    position = jnp.where(lane < hb, half_ref[own] * hb + lane, half_ref[own + 1] * hb + lane - hb)
    limit = jnp.zeros((8, T), jnp.int32)
    start = jnp.int32(0)
    for f in range(frame_ref.shape[0]):
        length = frame_ref[f]
        limit = limit + jnp.where(start <= position, length, 0)
        start = start + length
    limit = jnp.broadcast_to(limit[0:1], (T, T))
    row = lax.broadcasted_iota(jnp.int32, (T, T), 0)
    col = lax.broadcasted_iota(jnp.int32, (T, T), 1)
    eye = jnp.where(row == col, 1.0, 0.0).astype(jnp.bfloat16)
    vaug[:, HEAD_WIDTH:] = jnp.ones((vaug.shape[0], HEAD_WIDTH), jnp.bfloat16)

    def place(at, which, j):
        block = (lax.rem(s - j + S, S) * C + (c if which == 0 else other)) * 2
        place_at = jnp.where(row < hb, half_ref[block] * hb + row, half_ref[block + 1] * hb + row - hb)
        hidden = jnp.where(place_at < limit, 0.0, MASKED).astype(jnp.bfloat16)
        kaug[at * T : (at + 1) * T, :HEAD_WIDTH] = kv[which, j, 0]
        kaug[at * T : (at + 1) * T, HEAD_WIDTH:] = hidden
        vaug[at * T : (at + 1) * T, :HEAD_WIDTH] = kv[which, j, 1]

    tile = min(ROW_TILE, heads * T)

    def prepare(slots):
        for at, j in enumerate(slots):
            place(2 * at, 0, j)
            got(kv.at[1, j], ks_r.at[j])
            place(2 * at + 1, 1, j)

    def attend_rows(slots, first_tile, last_tile, opening=False):
        count = 2 * len(slots) * T

        for i in range(first_tile, last_tile):
            rows = slice(i * tile, (i + 1) * tile)
            scores = lax.dot_general(
                qaug[rows], kaug[:count], (((1,), (1,)), ((), ())), preferred_element_type=jnp.float32
            )
            top = jnp.max(scores, axis=1, keepdims=True)
            if opening:
                new = jnp.broadcast_to(top, (tile, HEAD_WIDTH))
            else:
                old = m_buf[rows]
                new = jnp.maximum(old, top)
            m_buf[rows] = new
            weights = jnp.exp2((scores - jnp.concatenate([new] * (count // HEAD_WIDTH), axis=1)) * SCALE_LOG2)
            product = jnp.dot(weights.astype(jnp.bfloat16), vaug[:count], preferred_element_type=jnp.float32)
            if opening:
                acc[rows] = product
            else:
                fade = jnp.exp2((old - new) * SCALE_LOG2)
                acc[rows] = acc[rows] * jnp.concatenate([fade, fade], axis=1) + product

    row_tiles = heads * T // tile
    mid_tile = row_tiles // 2

    def attend(slots, opening=False, between=None):
        prepare(slots)
        attend_rows(slots, 0, mid_tile, opening)
        if between is not None:
            between()
        attend_rows(slots, mid_tile, row_tiles, opening)

    rounds = H // 2

    def ring_signal(r):
        pl.semaphore_signal(ring_sem.at[0, r], inc=1, device_id={"heads": h_up}, device_id_type=MESH)
        pl.semaphore_signal(ring_sem.at[1, r], inc=1, device_id={"heads": h_down}, device_id_type=MESH)

    def ring_wait(r):
        pl.semaphore_wait(ring_sem.at[0, r], 1)
        pl.semaphore_wait(ring_sem.at[1, r], 1)

    pl.semaphore_wait(barrier, len(peers))
    ins[0].wait()
    key_right(0, 0)
    key_left(0, 0)
    ins[1].wait()
    key_right(0, 1)
    key_left(0, 1)
    key_across(0)
    ins[3].wait()
    own_w(0)
    ring_signal(0)
    ins[2].wait()
    for i in range(heads):
        qaug[i * T : (i + 1) * T, :HEAD_WIDTH] = q_buf[:, i * HEAD_WIDTH : (i + 1) * HEAD_WIDTH]
        qaug[i * T : (i + 1) * T, HEAD_WIDTH:] = eye

    def key_round(d, last):
        for i in range(2):
            got(kv.at[0, d, i], kz_r.at[d, i])
            if not last or i == 0:
                key_right(d, i)
            got(kv.at[0, S - d, i], kz_r.at[S - d, i])
            if not last or i == 1:
                key_left(d, i)
        key_across(d)
        key_across(S - d)
        own_w(d)

    def w_first(d, last=False):
        got(wbuf.at[d, first], w_r.at[d, 0])
        w_right(d, first, 0)
        w_pair(d)
        got(wbuf.at[S - d, first], w_r.at[S - d, 0])
        if not last:
            w_left(d, first, 0)
        w_pair(S - d)

    def w_second(d, last=False):
        got(wbuf.at[d, second], w_r.at[d, 1])
        if not last:
            w_right(d, second, 1)
        got(wbuf.at[S - d, second], w_r.at[S - d, 1])
        w_left(d, second, 1)

    def finish():
        for i in range(heads):
            rows = slice(i * T, (i + 1) * T)
            cols = slice(i * HEAD_WIDTH, (i + 1) * HEAD_WIDTH)
            attf[0, :, cols] = (acc[rows, :HEAD_WIDTH] / acc[rows, HEAD_WIDTH:]).astype(jnp.bfloat16)

    across = remote(attf.at[0], attf.at[1], a_s, a_r, {"sub": other})
    att_copy = pltpu.make_async_copy(attf.at[0], att_hbm, io_sem.at[6])

    def route(j):
        block = lax.rem(s - j + S, S)
        to = block // per
        return to, lax.rem(block, per), lax.rem(to - h + H, H)

    def deliver(j):
        to, turn, away = route(j)
        tile = turn * C + c
        remote(
            c_out.at[j, 0], c_in.at[away, tile], c_s.at[j, 0], c_r.at[away, tile], {"heads": to}
        ).start()
        remote(
            c_out.at[j, 1], c_in.at[away, tile], c_s.at[j, 1], c_r.at[away, tile], {"heads": to, "sub": other}
        ).start()

    def project(slots):
        both = jnp.concatenate([attf[0], attf[1]], axis=0)
        weights = jnp.concatenate([wbuf[j] for j in slots], axis=1)
        terms = jnp.dot(both, weights, preferred_element_type=jnp.float32).astype(jnp.bfloat16)
        for i, j in enumerate(slots):
            for t in range(2):
                c_out[j, t] = terms[t * T : (t + 1) * T, i * T : (i + 1) * T]

    def send_slot(j):
        turn, away = route(j)[1:]

        def hand(part, dst, send, recv, step):
            remote(part, dst, send, recv, {"heads": lax.rem(h + step + H, H)}).start()

        if merging:
            direct = jnp.logical_or(away == 1, away == H - 1)

            @pl.when(away == 3)
            def _():
                hand(c_out.at[j], m_in.at[0, turn], c_s.at[j, 0], m_r.at[0, turn], 1)

            @pl.when(away == 5)
            def _():
                hand(c_out.at[j], m_in.at[1, turn], c_s.at[j, 0], m_r.at[1, turn], -1)

            @pl.when(away == 4)
            def _():
                hand(c_out.at[j, 0], m_far.at[0, turn], c_s.at[j, 0], f_r.at[0, turn], 2)
                hand(c_out.at[j, 1], m_far.at[1, turn], c_s.at[j, 1], f_r.at[1, turn], -2)
        else:
            direct = away > 0

        @pl.when(direct)
        def _():
            deliver(j)

        @pl.when(away == 0)
        def _():
            tile = turn * C + c
            pltpu.make_async_copy(c_out.at[j, 0], c_in.at[0, tile], c_r.at[0, tile]).start()
            remote(c_out.at[j, 1], c_in.at[0, tile], c_s.at[j, 1], c_r.at[0, tile], {"sub": other}).start()

    def merge_sums(nearest, furthest):
        if not merging:
            return
        for side, away in enumerate((2, 6)):
            for turn in range(per):
                block = lax.rem(h + away, H) * per + turn
                j = lax.rem(s - block + S, S)
                planes = jnp.minimum(j, S - j)

                @pl.when(jnp.logical_and(planes >= nearest, planes <= furthest))
                def _(side=side, turn=turn, j=j):
                    got(m_in.at[side, turn], m_r.at[side, turn])
                    got(m_far.at[side, turn], f_r.at[side, turn])
                    near = m_in[side, turn].astype(jnp.float32)
                    far = m_far[side, turn].astype(jnp.float32)
                    for t in range(2):
                        total = c_out[j, t].astype(jnp.float32) + near[t]
                        if t == side:
                            total = total + far
                        c_out[j, t] = total.astype(jnp.bfloat16)
                    deliver(j)

    key_round(1, half == 2)
    attend([0], opening=True)

    def key_step(d, carry):
        @pl.when(d - 2 < rounds)
        def _():
            ring_wait(d - 2)

        @pl.when(d - 1 < rounds)
        def _():
            ring_signal(d - 1)

        key_round(d, False)

        def between():
            @pl.when(d > lag)
            def _():
                w_first(d - lag)

        attend([d - 1, S - d + 1], between=between)

        @pl.when(d > lag)
        def _():
            w_second(d - lag)

        return carry

    if half > 2:
        lax.fori_loop(2, half - 1, key_step, 0)
        key_round(half - 1, True)
        attend([half - 2, S - half + 2], between=(lambda: w_first(half - 1 - lag)) if half - 1 > lag else None)
        if half - 1 > lag:
            w_second(half - 1 - lag)
    for r in range(max(0, half - 3), rounds):
        ring_wait(r)
        if r + 1 < rounds:
            ring_signal(r + 1)
    got(kv.at[0, half, 0], kz_r.at[half, 0])
    got(kv.at[0, half, 1], kz_r.at[half, 1])
    key_across(half)
    at = half - lag
    attend([half - 1, S - half + 1], between=lambda: w_first(at, at == half - 1))
    w_second(at, at == half - 1)

    def closing():
        attend([half])
        finish()
        across.start()
        att_copy.start()

    groups = [[0]] + [[d, S - d] for d in range(1, half)] + [[half]]
    done = 0

    def catch_up(upto):
        nonlocal done
        while done < upto:
            for j in groups[done]:
                if j:
                    w_pair_got(j)
            project(groups[done])
            for j in groups[done]:
                send_slot(j)
            done += 1

    todo = [closing, lambda: (across.wait(), catch_up(max(1, half - lag)))]
    for d in range(half - lag + 1, half):
        w_first(d, d == half - 1)
        if todo:
            todo.pop(0)()
        else:
            catch_up(d - 1)
        w_second(d, d == half - 1)
    got(wbuf.at[half, first], w_r.at[half, 0])
    w_pair(half)
    while todo:
        todo.pop(0)()
    early = done - 1
    catch_up(half)
    got(wbuf.at[half, second], w_r.at[half, 1])
    catch_up(half + 1)
    merge_sums(0, early)
    merge_sums(early + 1, half)

    ins[4].wait()

    energy = jnp.zeros((T, 1), jnp.float32)
    tiles = c_in.shape[1]
    senders = (0, 1, 2, 6, 7) if merging else tuple(range(H))
    for t in range(tiles):
        cols = slice(t * T, (t + 1) * T)
        total = res_buf[:, cols].astype(jnp.float32)
        for p in senders:
            got(c_in.at[p, t], c_r.at[p, t])
        summed = c_in[0, t].astype(jnp.float32)
        for p in senders[1:]:
            summed = summed + c_in[p, t].astype(jnp.float32)
        state = (total + summed).astype(jnp.bfloat16)
        hid_buf[:, cols] = state
        wide = state.astype(jnp.float32)
        energy = energy + jnp.sum(wide * wide, axis=1, keepdims=True)
    e_out[...] = jnp.transpose(jnp.broadcast_to(energy, (T, T)))[:8]
    for i in range(1, H):
        to = lax.rem(h + i, H)
        remote(e_out, e_in.at[h], e_s.at[i], e_r.at[h], {"heads": to}).start()
    hid_copy = pltpu.make_async_copy(hid_buf, hid_hbm, io_sem.at[7])
    hid_copy.start()
    def drain_keys(d, carry):
        for i in range(2):
            for way in range(2):
                sent(kv.at[0, 0, i], kz_s.at[way, d, i])
        return carry

    lax.fori_loop(0, half - 1, drain_keys, 0)
    sent(kv.at[0, 0, 0], kz_s.at[0, half - 1, 0])
    sent(kv.at[0, 0, 1], kz_s.at[1, half - 1, 1])

    def drain_w(d, carry):
        for way in range(2):
            sent(wbuf.at[0, first], wz_s.at[way, d, 0])
            sent(wbuf.at[0, second], wz_s.at[way, d, 1])
        return carry

    lax.fori_loop(0, half - 1, drain_w, 0)
    sent(wbuf.at[0, first], wz_s.at[0, half - 1, 0])
    sent(wbuf.at[0, second], wz_s.at[1, half - 1, 1])

    def drain_slots(j, carry):
        sent(kv.at[0, 0], ks_s.at[j])
        away = route(j)[2]
        whole = jnp.logical_or(away == 3, away == 5) if merging else away < 0

        @pl.when(whole)
        def _():
            sent(c_out.at[0], c_s.at[j, 0])

        @pl.when(jnp.logical_not(whole))
        def _():
            sent(c_out.at[0, 1], c_s.at[j, 1])

            @pl.when(away > 0)
            def _():
                sent(c_out.at[0, 0], c_s.at[j, 0])

        if use_y:

            @pl.when(j > 0)
            def _():
                sent(wbuf.at[0, first], wy_s.at[j])

        return carry

    lax.fori_loop(0, S, drain_slots, 0)
    everyone = e_out[...]
    for i in range(1, H):
        of = lax.rem(h + i, H)
        got(e_in.at[of], e_r.at[of])
        everyone = everyone + e_in[of]
    e_sum[...] = everyone
    sum_copy = pltpu.make_async_copy(e_sum, sum_hbm, io_sem.at[8])
    sum_copy.start()
    for i in range(1, H):
        sent(e_out, e_s.at[i])
    att_copy.wait()
    hid_copy.wait()
    sum_copy.wait()


def norm(width, sum_hbm, gain_hbm, att_hbm, hid_hbm, att_out, hid_out, norm_out, e_sum, gain, att, hid, normed, sems):
    T, cols = hid.shape
    pairs = ((att_hbm, att), (hid_hbm, hid), (sum_hbm, e_sum), (gain_hbm, gain))
    ins = [pltpu.make_async_copy(a, b, sems.at[i]) for i, (a, b) in enumerate(pairs)]
    for copy in ins:
        copy.start()
    outs = [
        pltpu.make_async_copy(a, b, sems.at[4 + i])
        for i, (a, b) in enumerate(((att, att_out), (hid, hid_out), (normed, norm_out)))
    ]
    ins[0].wait()
    outs[0].start()
    ins[1].wait()
    outs[1].start()
    ins[2].wait()
    ins[3].wait()
    mean = jnp.transpose(jnp.broadcast_to(e_sum[0:1], (T, T))) * (1.0 / width)
    factor = lax.rsqrt(mean + 1e-6)
    for t in range(cols // T):
        at = slice(t * T, (t + 1) * T)
        normed[:, at] = (hid[:, at].astype(jnp.float32) * factor * gain[:, at]).astype(jnp.bfloat16)
    outs[2].start()
    for copy in outs:
        copy.wait()


def shards(sizes, queries, keys, values, half_order, frame_lengths, out_proj, residual_in, norm_gain):
    G, S, H, C = sizes
    T, width = queries.shape
    K, cols = out_proj.shape
    tiles = residual_in.shape[1] // cols
    heads = width // HEAD_WIDTH
    bf16, f32, dma = jnp.bfloat16, jnp.float32, pltpu.SemaphoreType.DMA
    anywhere = pl.BlockSpec(memory_space=pl.ANY)
    smem = pl.BlockSpec(memory_space=pltpu.SMEM)
    attended, hidden, sums = pl.pallas_call(
        functools.partial(fused, sizes),
        out_shape=(
            jax.ShapeDtypeStruct(queries.shape, bf16),
            jax.ShapeDtypeStruct(residual_in.shape, bf16),
            jax.ShapeDtypeStruct((8, T), f32),
        ),
        in_specs=[smem, smem] + [anywhere] * 5,
        out_specs=(anywhere,) * 3,
        scratch_shapes=[
            pltpu.VMEM((T, width), bf16),
            pltpu.VMEM((heads * T, 2 * HEAD_WIDTH), bf16),
            pltpu.VMEM((2, S, 2, T, HEAD_WIDTH), bf16),
            pltpu.VMEM((4 * T, 2 * HEAD_WIDTH), bf16),
            pltpu.VMEM((4 * T, 2 * HEAD_WIDTH), bf16),
            pltpu.VMEM((heads * T, HEAD_WIDTH), f32),
            pltpu.VMEM((heads * T, 2 * HEAD_WIDTH), f32),
            pltpu.VMEM((2, T, width), bf16),
            pltpu.VMEM((S, K, cols), bf16),
            pltpu.VMEM((S, 2, T, cols), bf16),
            pltpu.VMEM((H, tiles, T, cols), bf16),
            pltpu.VMEM((2, S // H, 2, T, cols), bf16),
            pltpu.VMEM((2, S // H, T, cols), bf16),
            pltpu.VMEM(residual_in.shape, bf16),
            pltpu.VMEM(residual_in.shape, bf16),
            pltpu.VMEM((8, T), f32),
            pltpu.VMEM((H, 8, T), f32),
            pltpu.VMEM((8, T), f32),
            dma((9,)),
            pltpu.SemaphoreType.REGULAR((2, H // 2)),
            dma((2, S // 2, 2)),
            dma((S, 2)),
            dma((S,)),
            dma((S,)),
            dma((2, S // 2, 2)),
            dma((S, 3)),
            dma((S,)),
            dma((S, 2)),
            dma((H, tiles)),
            dma((2, S // H)),
            dma((2, S // H)),
            dma(()),
            dma(()),
            dma((H,)),
            dma((H,)),
        ],
        compiler_params=pltpu.CompilerParams(collective_id=0, has_side_effects=True),
    )(half_order, frame_lengths, queries, keys, values, out_proj, residual_in)
    return pl.pallas_call(
        functools.partial(norm, residual_in.shape[1] * H),
        out_shape=(
            jax.ShapeDtypeStruct(queries.shape, bf16),
            jax.ShapeDtypeStruct(residual_in.shape, bf16),
            jax.ShapeDtypeStruct(residual_in.shape, bf16),
        ),
        in_specs=[anywhere] * 4,
        out_specs=(anywhere,) * 3,
        scratch_shapes=[
            pltpu.VMEM((8, T), f32),
            pltpu.VMEM((1, residual_in.shape[1]), f32),
            pltpu.VMEM((T, width), bf16),
            pltpu.VMEM(residual_in.shape, bf16),
            pltpu.VMEM(residual_in.shape, bf16),
            dma((7,)),
        ],
    )(sums, norm_gain.reshape(1, -1), attended, hidden)


def solution(mesh):
    sizes = tuple(mesh.shape[a] for a in ("groups", "seq", "heads", "sub"))
    rows = P(("groups", "seq", "sub"), "heads")
    in_specs = (rows, rows, rows, P("groups"), P("groups"), P("heads", ("seq", "sub")), rows, P("heads"))
    return jax.shard_map(
        functools.partial(shards, sizes), mesh=mesh, in_specs=in_specs, out_specs=(rows,) * 3, check_vma=False
    )
```

```python
import functools

import jax
import jax.numpy as jnp
from jax import lax
from jax.experimental import pallas as pl
from jax.experimental.pallas import tpu as pltpu
from jax.sharding import PartitionSpec as P

HEAD_WIDTH = 128
MASKED = -1e30
SCALE_LOG2 = HEAD_WIDTH ** (-0.5) * 1.4426950408889634
MESH = pl.DeviceIdType.MESH
ROW_TILE = 256
Y_ROWS = 6
LAG = 2


def fused(
    sizes,
    half_ref,
    frame_ref,
    q_hbm,
    k_hbm,
    v_hbm,
    w_hbm,
    res_hbm,
    att_hbm,
    hid_hbm,
    sum_hbm,
    q_buf,
    qaug,
    kv,
    kaug,
    vaug,
    m_buf,
    acc,
    attf,
    wbuf,
    c_out,
    c_in,
    m_in,
    m_far,
    res_buf,
    hid_buf,
    e_out,
    e_in,
    e_sum,
    io_sem,
    ring_sem,
    kz_s,
    kz_r,
    ks_s,
    ks_r,
    wz_s,
    w_r,
    wy_s,
    c_s,
    c_r,
    m_r,
    f_r,
    a_s,
    a_r,
    e_s,
    e_r,
):
    G, S, H, C = sizes
    use_y = G % 2 == 0
    half = S // 2
    lag = max(1, half * LAG // 8)
    per = S // H
    merging = H == 8
    T = q_buf.shape[0]
    K = wbuf.shape[1]
    heads = q_buf.shape[1] // HEAD_WIDTH
    hb = T // 2
    g, s, h, c = (lax.axis_index(a) for a in ("groups", "seq", "heads", "sub"))
    right, left = lax.rem(s + 1, S), lax.rem(s + S - 1, S)
    other = 1 - c

    ins = [
        pltpu.make_async_copy(k_hbm, kv.at[0, 0, 0], io_sem.at[0]),
        pltpu.make_async_copy(v_hbm, kv.at[0, 0, 1], io_sem.at[1]),
        pltpu.make_async_copy(q_hbm, q_buf, io_sem.at[2]),
        pltpu.make_async_copy(w_hbm, wbuf.at[0], io_sem.at[3]),
        pltpu.make_async_copy(res_hbm, res_buf, io_sem.at[4]),
    ]
    for copy in ins:
        copy.start()

    barrier = pltpu.get_barrier_semaphore()
    peers = [{"seq": left}, {"seq": right}, {"sub": other}]
    if use_y:
        parity = lax.rem(g, 2)
        partner = g + 1 - 2 * parity
        peers.append({"groups": partner})
    h_up, h_down = lax.rem(h + 1, H), lax.rem(h + H - 1, H)
    peers += [{"heads": h_up}, {"heads": h_down}]
    for peer in peers:
        pl.semaphore_signal(barrier, inc=1, device_id=peer, device_id_type=MESH)

    if use_y:
        part = K * Y_ROWS // 16
        first = pl.ds(pl.multiple_of(parity * (K - part), 16), part)
        second = pl.ds(part, K - 2 * part)
        third = pl.ds(pl.multiple_of((1 - parity) * (K - part), 16), part)
        first_at = pl.multiple_of(parity * (K - part), 16)
    else:
        part = K // 2
        first = pl.ds(0, part)
        second = pl.ds(part, K - part)
        third = None
        first_at = 0
    second_rows = K - 2 * part if use_y else K - part
    pieces = max(1, half // 4)

    def remote(src, dst, send, recv, device):
        return pltpu.make_async_remote_copy(
            src_ref=src, dst_ref=dst, send_sem=send, recv_sem=recv, device_id=device, device_id_type=MESH
        )

    def got(ref, sem):
        remote(ref, ref, a_s, sem, {"sub": other}).wait_recv()

    def sent(ref, sem):
        remote(ref, ref, sem, a_r, {"sub": other}).wait_send()

    def key_right(d, i):
        remote(kv.at[0, d, i], kv.at[0, d + 1, i], kz_s.at[0, d, i], kz_r.at[d + 1, i], {"seq": right}).start()

    def key_left(d, i):
        at = lax.rem(S - d, S)
        remote(kv.at[0, at, i], kv.at[0, S - d - 1, i], kz_s.at[1, d, i], kz_r.at[S - d - 1, i], {"seq": left}).start()

    def key_across(j):
        remote(kv.at[0, j], kv.at[1, j], ks_s.at[j], ks_r.at[j], {"sub": other}).start()

    def own_w(d):
        def send(at, rows, sub):
            ds = pl.ds(pl.multiple_of(at, 16), rows)
            remote(wbuf.at[0, ds], wbuf.at[1, ds], wz_s.at[0, 0, sub], w_r.at[1, sub], {"seq": right}).start()
            remote(wbuf.at[0, ds], wbuf.at[S - 1, ds], wz_s.at[1, 0, sub], w_r.at[S - 1, sub], {"seq": left}).start()

        @pl.when(d < pieces)
        def _():
            send(first_at + d * (part // pieces), part // pieces, 0)

        @pl.when(jnp.logical_and(d >= pieces, d < 2 * pieces))
        def _():
            send(part + (d - pieces) * (second_rows // pieces), second_rows // pieces, 1)

    def w_right(d, rows, sub):
        remote(wbuf.at[d, rows], wbuf.at[d + 1, rows], wz_s.at[0, d, sub], w_r.at[d + 1, sub], {"seq": right}).start()

    def w_left(d, rows, sub):
        remote(
            wbuf.at[S - d, rows], wbuf.at[S - d - 1, rows], wz_s.at[1, d, sub], w_r.at[S - d - 1, sub], {"seq": left}
        ).start()

    def w_pair(j):
        if use_y:
            remote(wbuf.at[j, first], wbuf.at[j, first], wy_s.at[j], w_r.at[j, 2], {"groups": partner}).start()

    def w_pair_got(j):
        if use_y:
            got(wbuf.at[j, third], w_r.at[j, 2])

    lane = lax.broadcasted_iota(jnp.int32, (8, T), 1)
    own = (s * C + c) * 2
    position = jnp.where(lane < hb, half_ref[own] * hb + lane, half_ref[own + 1] * hb + lane - hb)
    limit = jnp.zeros((8, T), jnp.int32)
    start = jnp.int32(0)
    for f in range(frame_ref.shape[0]):
        length = frame_ref[f]
        limit = limit + jnp.where(start <= position, length, 0)
        start = start + length
    limit = jnp.broadcast_to(limit[0:1], (T, T))
    row = lax.broadcasted_iota(jnp.int32, (T, T), 0)
    col = lax.broadcasted_iota(jnp.int32, (T, T), 1)
    eye = jnp.where(row == col, 1.0, 0.0).astype(jnp.bfloat16)
    vaug[:, HEAD_WIDTH:] = jnp.ones((vaug.shape[0], HEAD_WIDTH), jnp.bfloat16)

    def place(at, which, j):
        block = (lax.rem(s - j + S, S) * C + (c if which == 0 else other)) * 2
        place_at = jnp.where(row < hb, half_ref[block] * hb + row, half_ref[block + 1] * hb + row - hb)
        hidden = jnp.where(place_at < limit, 0.0, MASKED).astype(jnp.bfloat16)
        kaug[at * T : (at + 1) * T, :HEAD_WIDTH] = kv[which, j, 0]
        kaug[at * T : (at + 1) * T, HEAD_WIDTH:] = hidden
        vaug[at * T : (at + 1) * T, :HEAD_WIDTH] = kv[which, j, 1]

    tile = min(ROW_TILE, heads * T)

    def prepare(slots):
        for at, j in enumerate(slots):
            place(2 * at, 0, j)
            got(kv.at[1, j], ks_r.at[j])
            place(2 * at + 1, 1, j)

    def attend_rows(slots, first_tile, last_tile, opening=False):
        count = 2 * len(slots) * T

        for i in range(first_tile, last_tile):
            rows = slice(i * tile, (i + 1) * tile)
            scores = lax.dot_general(
                qaug[rows], kaug[:count], (((1,), (1,)), ((), ())), preferred_element_type=jnp.float32
            )
            top = jnp.max(scores, axis=1, keepdims=True)
            if opening:
                new = jnp.broadcast_to(top, (tile, HEAD_WIDTH))
            else:
                old = m_buf[rows]
                new = jnp.maximum(old, top)
            m_buf[rows] = new
            weights = jnp.exp2((scores - jnp.concatenate([new] * (count // HEAD_WIDTH), axis=1)) * SCALE_LOG2)
            product = jnp.dot(weights.astype(jnp.bfloat16), vaug[:count], preferred_element_type=jnp.float32)
            if opening:
                acc[rows] = product
            else:
                fade = jnp.exp2((old - new) * SCALE_LOG2)
                acc[rows] = acc[rows] * jnp.concatenate([fade, fade], axis=1) + product

    row_tiles = heads * T // tile
    mid_tile = row_tiles // 2

    def attend(slots, opening=False, between=None):
        prepare(slots)
        attend_rows(slots, 0, mid_tile, opening)
        if between is not None:
            between()
        attend_rows(slots, mid_tile, row_tiles, opening)

    rounds = H // 2

    def ring_signal(r):
        pl.semaphore_signal(ring_sem.at[0, r], inc=1, device_id={"heads": h_up}, device_id_type=MESH)
        pl.semaphore_signal(ring_sem.at[1, r], inc=1, device_id={"heads": h_down}, device_id_type=MESH)

    def ring_wait(r):
        pl.semaphore_wait(ring_sem.at[0, r], 1)
        pl.semaphore_wait(ring_sem.at[1, r], 1)

    pl.semaphore_wait(barrier, len(peers))
    ins[0].wait()
    key_right(0, 0)
    key_left(0, 0)
    ins[1].wait()
    key_right(0, 1)
    key_left(0, 1)
    key_across(0)
    ins[3].wait()
    own_w(0)
    ring_signal(0)
    ins[2].wait()
    for i in range(heads):
        qaug[i * T : (i + 1) * T, :HEAD_WIDTH] = q_buf[:, i * HEAD_WIDTH : (i + 1) * HEAD_WIDTH]
        qaug[i * T : (i + 1) * T, HEAD_WIDTH:] = eye

    def key_round(d, last):
        for i in range(2):
            got(kv.at[0, d, i], kz_r.at[d, i])
            if not last or i == 0:
                key_right(d, i)
            got(kv.at[0, S - d, i], kz_r.at[S - d, i])
            if not last or i == 1:
                key_left(d, i)
        key_across(d)
        key_across(S - d)
        own_w(d)

    def w_first(d, last=False):
        got(wbuf.at[d, first], w_r.at[d, 0])
        w_right(d, first, 0)
        w_pair(d)
        got(wbuf.at[S - d, first], w_r.at[S - d, 0])
        if not last:
            w_left(d, first, 0)
        w_pair(S - d)

    def w_second(d, last=False):
        got(wbuf.at[d, second], w_r.at[d, 1])
        if not last:
            w_right(d, second, 1)
        got(wbuf.at[S - d, second], w_r.at[S - d, 1])
        w_left(d, second, 1)

    def finish():
        for i in range(heads):
            rows = slice(i * T, (i + 1) * T)
            cols = slice(i * HEAD_WIDTH, (i + 1) * HEAD_WIDTH)
            attf[0, :, cols] = (acc[rows, :HEAD_WIDTH] / acc[rows, HEAD_WIDTH:]).astype(jnp.bfloat16)

    across = remote(attf.at[0], attf.at[1], a_s, a_r, {"sub": other})
    att_copy = pltpu.make_async_copy(attf.at[0], att_hbm, io_sem.at[6])

    def route(j):
        block = lax.rem(s - j + S, S)
        to = block // per
        return to, lax.rem(block, per), lax.rem(to - h + H, H)

    def deliver(j):
        to, turn, away = route(j)
        tile = turn * C + c
        remote(
            c_out.at[j, 0], c_in.at[away, tile], c_s.at[j, 0], c_r.at[away, tile], {"heads": to}
        ).start()
        remote(
            c_out.at[j, 1], c_in.at[away, tile], c_s.at[j, 1], c_r.at[away, tile], {"heads": to, "sub": other}
        ).start()

    def project(slots):
        both = jnp.concatenate([attf[0], attf[1]], axis=0)
        weights = jnp.concatenate([wbuf[j] for j in slots], axis=1)
        terms = jnp.dot(both, weights, preferred_element_type=jnp.float32).astype(jnp.bfloat16)
        for i, j in enumerate(slots):
            for t in range(2):
                c_out[j, t] = terms[t * T : (t + 1) * T, i * T : (i + 1) * T]

    def send_slot(j):
        turn, away = route(j)[1:]

        def hand(part, dst, send, recv, step):
            remote(part, dst, send, recv, {"heads": lax.rem(h + step + H, H)}).start()

        if merging:
            direct = jnp.logical_or(away == 1, away == H - 1)

            @pl.when(away == 3)
            def _():
                hand(c_out.at[j], m_in.at[0, turn], c_s.at[j, 0], m_r.at[0, turn], 1)

            @pl.when(away == 5)
            def _():
                hand(c_out.at[j], m_in.at[1, turn], c_s.at[j, 0], m_r.at[1, turn], -1)

            @pl.when(away == 4)
            def _():
                hand(c_out.at[j, 0], m_far.at[0, turn], c_s.at[j, 0], f_r.at[0, turn], 2)
                hand(c_out.at[j, 1], m_far.at[1, turn], c_s.at[j, 1], f_r.at[1, turn], -2)
        else:
            direct = away > 0

        @pl.when(direct)
        def _():
            deliver(j)

        @pl.when(away == 0)
        def _():
            tile = turn * C + c
            pltpu.make_async_copy(c_out.at[j, 0], c_in.at[0, tile], c_r.at[0, tile]).start()
            remote(c_out.at[j, 1], c_in.at[0, tile], c_s.at[j, 1], c_r.at[0, tile], {"sub": other}).start()

    def merge_sums(nearest, furthest):
        if not merging:
            return
        for side, away in enumerate((2, 6)):
            for turn in range(per):
                block = lax.rem(h + away, H) * per + turn
                j = lax.rem(s - block + S, S)
                planes = jnp.minimum(j, S - j)

                @pl.when(jnp.logical_and(planes >= nearest, planes <= furthest))
                def _(side=side, turn=turn, j=j):
                    got(m_in.at[side, turn], m_r.at[side, turn])
                    got(m_far.at[side, turn], f_r.at[side, turn])
                    near = m_in[side, turn].astype(jnp.float32)
                    far = m_far[side, turn].astype(jnp.float32)
                    for t in range(2):
                        total = c_out[j, t].astype(jnp.float32) + near[t]
                        if t == side:
                            total = total + far
                        c_out[j, t] = total.astype(jnp.bfloat16)
                    deliver(j)

    key_round(1, half == 2)
    attend([0], opening=True)

    def key_step(d, carry):
        @pl.when(d - 2 < rounds)
        def _():
            ring_wait(d - 2)

        @pl.when(d - 1 < rounds)
        def _():
            ring_signal(d - 1)

        key_round(d, False)

        def between():
            @pl.when(d > lag)
            def _():
                w_first(d - lag)

        attend([d - 1, S - d + 1], between=between)

        @pl.when(d > lag)
        def _():
            w_second(d - lag)

        return carry

    if half > 2:
        lax.fori_loop(2, half - 1, key_step, 0)
        key_round(half - 1, True)
        attend([half - 2, S - half + 2], between=(lambda: w_first(half - 1 - lag)) if half - 1 > lag else None)
        if half - 1 > lag:
            w_second(half - 1 - lag)
    for r in range(max(0, half - 3), rounds):
        ring_wait(r)
        if r + 1 < rounds:
            ring_signal(r + 1)
    got(kv.at[0, half, 0], kz_r.at[half, 0])
    got(kv.at[0, half, 1], kz_r.at[half, 1])
    key_across(half)
    at = half - lag
    attend([half - 1, S - half + 1], between=lambda: w_first(at, at == half - 1))
    w_second(at, at == half - 1)

    def closing():
        attend([half])
        finish()
        across.start()
        att_copy.start()

    groups = [[0]] + [[d, S - d] for d in range(1, half)] + [[half]]
    done = 0

    def catch_up(upto):
        nonlocal done
        while done < upto:
            for j in groups[done]:
                if j:
                    w_pair_got(j)
            project(groups[done])
            for j in groups[done]:
                send_slot(j)
            done += 1

    todo = [closing, lambda: (across.wait(), catch_up(max(1, half - lag)))]
    for d in range(half - lag + 1, half):
        w_first(d, d == half - 1)
        if todo:
            todo.pop(0)()
        else:
            catch_up(d - 1)
        w_second(d, d == half - 1)
    got(wbuf.at[half, first], w_r.at[half, 0])
    w_pair(half)
    while todo:
        todo.pop(0)()
    early = done - 1
    catch_up(half)
    got(wbuf.at[half, second], w_r.at[half, 1])
    catch_up(half + 1)
    merge_sums(0, early)
    merge_sums(early + 1, half)

    ins[4].wait()

    energy = jnp.zeros((T, 1), jnp.float32)
    tiles = c_in.shape[1]
    senders = (0, 1, 2, 6, 7) if merging else tuple(range(H))
    for t in range(tiles):
        cols = slice(t * T, (t + 1) * T)
        total = res_buf[:, cols].astype(jnp.float32)
        for p in senders:
            got(c_in.at[p, t], c_r.at[p, t])
        summed = c_in[0, t].astype(jnp.float32)
        for p in senders[1:]:
            summed = summed + c_in[p, t].astype(jnp.float32)
        state = (total + summed).astype(jnp.bfloat16)
        hid_buf[:, cols] = state
        wide = state.astype(jnp.float32)
        energy = energy + jnp.sum(wide * wide, axis=1, keepdims=True)
    e_out[...] = jnp.transpose(jnp.broadcast_to(energy, (T, T)))[:8]
    for i in range(1, H):
        to = lax.rem(h + i, H)
        remote(e_out, e_in.at[h], e_s.at[i], e_r.at[h], {"heads": to}).start()
    hid_copy = pltpu.make_async_copy(hid_buf, hid_hbm, io_sem.at[7])
    hid_copy.start()
    def drain_keys(d, carry):
        for i in range(2):
            for way in range(2):
                sent(kv.at[0, 0, i], kz_s.at[way, d, i])
        return carry

    lax.fori_loop(0, half - 1, drain_keys, 0)
    sent(kv.at[0, 0, 0], kz_s.at[0, half - 1, 0])
    sent(kv.at[0, 0, 1], kz_s.at[1, half - 1, 1])

    def drain_w(d, carry):
        for way in range(2):
            sent(wbuf.at[0, first], wz_s.at[way, d, 0])
            sent(wbuf.at[0, second], wz_s.at[way, d, 1])
        return carry

    lax.fori_loop(0, half - 1, drain_w, 0)
    sent(wbuf.at[0, first], wz_s.at[0, half - 1, 0])
    sent(wbuf.at[0, second], wz_s.at[1, half - 1, 1])

    def drain_slots(j, carry):
        sent(kv.at[0, 0], ks_s.at[j])
        away = route(j)[2]
        whole = jnp.logical_or(away == 3, away == 5) if merging else away < 0

        @pl.when(whole)
        def _():
            sent(c_out.at[0], c_s.at[j, 0])

        @pl.when(jnp.logical_not(whole))
        def _():
            sent(c_out.at[0, 1], c_s.at[j, 1])

            @pl.when(away > 0)
            def _():
                sent(c_out.at[0, 0], c_s.at[j, 0])

        if use_y:

            @pl.when(j > 0)
            def _():
                sent(wbuf.at[0, first], wy_s.at[j])

        return carry

    lax.fori_loop(0, S, drain_slots, 0)
    everyone = e_out[...]
    for i in range(1, H):
        of = lax.rem(h + i, H)
        got(e_in.at[of], e_r.at[of])
        everyone = everyone + e_in[of]
    e_sum[...] = everyone
    sum_copy = pltpu.make_async_copy(e_sum, sum_hbm, io_sem.at[8])
    sum_copy.start()
    for i in range(1, H):
        sent(e_out, e_s.at[i])
    att_copy.wait()
    hid_copy.wait()
    sum_copy.wait()


def norm(width, sum_hbm, gain_hbm, att_hbm, hid_hbm, att_out, hid_out, norm_out, e_sum, gain, att, hid, normed, sems):
    T, cols = hid.shape
    pairs = ((att_hbm, att), (hid_hbm, hid), (sum_hbm, e_sum), (gain_hbm, gain))
    ins = [pltpu.make_async_copy(a, b, sems.at[i]) for i, (a, b) in enumerate(pairs)]
    for copy in ins:
        copy.start()
    outs = [
        pltpu.make_async_copy(a, b, sems.at[4 + i])
        for i, (a, b) in enumerate(((att, att_out), (hid, hid_out), (normed, norm_out)))
    ]
    ins[0].wait()
    outs[0].start()
    ins[1].wait()
    outs[1].start()
    ins[2].wait()
    ins[3].wait()
    mean = jnp.transpose(jnp.broadcast_to(e_sum[0:1], (T, T))) * (1.0 / width)
    factor = lax.rsqrt(mean + 1e-6)
    for t in range(cols // T):
        at = slice(t * T, (t + 1) * T)
        normed[:, at] = (hid[:, at].astype(jnp.float32) * factor * gain[:, at]).astype(jnp.bfloat16)
    outs[2].start()
    for copy in outs:
        copy.wait()


def shards(sizes, queries, keys, values, half_order, frame_lengths, out_proj, residual_in, norm_gain):
    G, S, H, C = sizes
    T, width = queries.shape
    K, cols = out_proj.shape
    tiles = residual_in.shape[1] // cols
    heads = width // HEAD_WIDTH
    bf16, f32, dma = jnp.bfloat16, jnp.float32, pltpu.SemaphoreType.DMA
    anywhere = pl.BlockSpec(memory_space=pl.ANY)
    smem = pl.BlockSpec(memory_space=pltpu.SMEM)
    attended, hidden, sums = pl.pallas_call(
        functools.partial(fused, sizes),
        out_shape=(
            jax.ShapeDtypeStruct(queries.shape, bf16),
            jax.ShapeDtypeStruct(residual_in.shape, bf16),
            jax.ShapeDtypeStruct((8, T), f32),
        ),
        in_specs=[smem, smem] + [anywhere] * 5,
        out_specs=(anywhere,) * 3,
        scratch_shapes=[
            pltpu.VMEM((T, width), bf16),
            pltpu.VMEM((heads * T, 2 * HEAD_WIDTH), bf16),
            pltpu.VMEM((2, S, 2, T, HEAD_WIDTH), bf16),
            pltpu.VMEM((4 * T, 2 * HEAD_WIDTH), bf16),
            pltpu.VMEM((4 * T, 2 * HEAD_WIDTH), bf16),
            pltpu.VMEM((heads * T, HEAD_WIDTH), f32),
            pltpu.VMEM((heads * T, 2 * HEAD_WIDTH), f32),
            pltpu.VMEM((2, T, width), bf16),
            pltpu.VMEM((S, K, cols), bf16),
            pltpu.VMEM((S, 2, T, cols), bf16),
            pltpu.VMEM((H, tiles, T, cols), bf16),
            pltpu.VMEM((2, S // H, 2, T, cols), bf16),
            pltpu.VMEM((2, S // H, T, cols), bf16),
            pltpu.VMEM(residual_in.shape, bf16),
            pltpu.VMEM(residual_in.shape, bf16),
            pltpu.VMEM((8, T), f32),
            pltpu.VMEM((H, 8, T), f32),
            pltpu.VMEM((8, T), f32),
            dma((9,)),
            pltpu.SemaphoreType.REGULAR((2, H // 2)),
            dma((2, S // 2, 2)),
            dma((S, 2)),
            dma((S,)),
            dma((S,)),
            dma((2, S // 2, 2)),
            dma((S, 3)),
            dma((S,)),
            dma((S, 2)),
            dma((H, tiles)),
            dma((2, S // H)),
            dma((2, S // H)),
            dma(()),
            dma(()),
            dma((H,)),
            dma((H,)),
        ],
        compiler_params=pltpu.CompilerParams(collective_id=0, has_side_effects=True),
    )(half_order, frame_lengths, queries, keys, values, out_proj, residual_in)
    return pl.pallas_call(
        functools.partial(norm, residual_in.shape[1] * H),
        out_shape=(
            jax.ShapeDtypeStruct(queries.shape, bf16),
            jax.ShapeDtypeStruct(residual_in.shape, bf16),
            jax.ShapeDtypeStruct(residual_in.shape, bf16),
        ),
        in_specs=[anywhere] * 4,
        out_specs=(anywhere,) * 3,
        scratch_shapes=[
            pltpu.VMEM((8, T), f32),
            pltpu.VMEM((1, residual_in.shape[1]), f32),
            pltpu.VMEM((T, width), bf16),
            pltpu.VMEM(residual_in.shape, bf16),
            pltpu.VMEM(residual_in.shape, bf16),
            dma((7,)),
        ],
    )(sums, norm_gain.reshape(1, -1), attended, hidden)


def solution(mesh):
    sizes = tuple(mesh.shape[a] for a in ("groups", "seq", "heads", "sub"))
    rows = P(("groups", "seq", "sub"), "heads")
    in_specs = (rows, rows, rows, P("groups"), P("groups"), P("heads", ("seq", "sub")), rows, P("heads"))
    return jax.shard_map(
        functools.partial(shards, sizes), mesh=mesh, in_specs=in_specs, out_specs=(rows,) * 3, check_vma=False
    )
```
